128 devices in a mesh: dp: 16 (over y_hi, x, core), mp: 8 (over y_lo, z).
Axes of the slice: x: 4, y: 4 (y_hi: 2, y_lo: 2; y = y_hi * 2 + y_lo), z: 4, core: 2. Of those that a mesh axis runs over, the one named last changes fastest.
Arguments:
- activations: bfloat16 [16384, 8192], P('dp'), may hold values from -18 to 18
- curvature: float32 [16384, 2048], P('dp', 'mp'), may hold values from 0.05 to 5
- basis: float32 [12, 16777216], P(None, ('dp', 'mp')), may hold values from -6 to 6
- krylov: float32 [16777216], P(('dp', 'mp')), may hold values from -38 to 38
Outputs:
- new_vector: float32 [16777216], P(('dp', 'mp'))
- hessenberg: float32 [13], replicated
The draws below stay inside these ranges and needn't reach their ends.
All inputs are finite; a program needn't handle non-finite values.
Results may differ from the reference program's by a relative error of at most 0.0058.
Values may be sent and summed in bfloat16 or wider, within the bound.
A program may use at most 128 MiB of HBM per device.

```python
import math
import jax
import jax.numpy as jnp
from jax import lax

D = 8192
BASIS = 12
KV = 1024
PARAMS = 16777216
TOKENS = 16384


def basis_row_stack(key):
    return jax.random.truncated_normal(jax.random.fold_in(key, 7), -6.0, 6.0, (BASIS, PARAMS), jnp.float32)


def draw_basis(key, part):
    return basis_row_stack(key)


def draw_krylov(key, part):
    stored = basis_row_stack(key)
    mixing = jax.random.uniform(jax.random.fold_in(key, 8), (BASIS,), jnp.float32, 0.5, 1.5)
    polarity = jnp.where(jax.random.normal(jax.random.fold_in(key, 9), (BASIS,), jnp.float32) > 0.0, 1.0, -1.0)
    noise_part = jax.random.truncated_normal(jax.random.fold_in(key, 10), -6.0, 6.0, (PARAMS,), jnp.float32)
    return (jnp.dot(mixing * polarity, stored, precision=lax.Precision.HIGHEST) + 0.6 * noise_part) / 3.0


def draw_activations(key, part):
    feature_scale = jnp.exp(jax.random.uniform(jax.random.fold_in(key, 3), (D,), jnp.float32, math.log(0.3), math.log(3.0)))
    values = jax.random.truncated_normal(jax.random.fold_in(key, 4), -6.0, 6.0, (TOKENS, D), jnp.float32)
    return (values * feature_scale[None, :]).astype(jnp.bfloat16)


def shard_levels(stream_key, extent, pieces, smallest, largest):
    level = 1.0
    for dim, shards_of in pieces:
        heights = jax.random.uniform(jax.random.fold_in(jax.random.fold_in(stream_key, 6), dim), (shards_of,), jnp.float32, smallest / len(pieces), largest / len(pieces))
        level = level * jnp.repeat(jnp.exp(heights), extent[dim] // shards_of).reshape((-1,) + (1,) * (len(extent) - 1 - dim))
    return level


def setup_inputs(seed: int = 0) -> dict:
    seeds = jax.random.split(jax.random.key(seed), 5)
    activations = draw_activations(jax.random.fold_in(seeds[4], 71), 0)
    curvature = jnp.clip(jnp.exp(math.log(5.0) - 4.6051702 * jax.random.uniform(seeds[1], (TOKENS, 2 * KV), jnp.float32) ** shard_levels(seeds[1], (TOKENS, 2 * KV), ((0, 16), (1, 8)), -0.2, 0.2)), 0.05, 5.0)
    basis = draw_basis(jax.random.fold_in(seeds[4], 71), 0)
    krylov = draw_krylov(jax.random.fold_in(seeds[4], 71), 0)
    return dict(activations=activations, curvature=curvature, basis=basis, krylov=krylov)


def reference(activations, curvature, basis, krylov):
    low_vector = krylov.astype(jnp.bfloat16).reshape(D, 2 * KV)
    projected_coefficients = jnp.dot(activations, low_vector, preferred_element_type=jnp.float32)
    weighted = (curvature * projected_coefficients).astype(jnp.bfloat16)
    gradient = lax.dot_general(activations, weighted, (((0,), (0,)), ((), ())), preferred_element_type=jnp.float32)
    curved = (gradient / TOKENS).reshape(PARAMS)
    coeffs = jnp.dot(basis, curved, precision=lax.Precision.HIGHEST) / PARAMS
    residual_vector = curved - jnp.dot(coeffs, basis, precision=lax.Precision.HIGHEST)
    mean_square = jnp.sum(residual_vector * residual_vector) / PARAMS
    scale_norm = jnp.sqrt(mean_square + 1e-06)
    return (residual_vector / scale_norm, jnp.concatenate([coeffs, scale_norm[None]]))
```

```python
import jax
import jax.numpy as jnp
from jax import lax
from jax.experimental import pallas as pl
from jax.experimental.pallas import tpu as pltpu
from jax.sharding import PartitionSpec as P

MESH = pl.DeviceIdType.MESH
TOKENS = 16384
PARAMS = 16777216
NB = 12
F32 = jnp.float32
BF16 = jnp.bfloat16
BLK = 256


def kernel(
    act_hbm, curv_hbm, basis_hbm, kry_ref, out_ref, hess_ref,
    act, curv, basis, vmat, ksend, zoth, acc, wt,
    dsend, drecv, xfs, xns, xfr, xl, xr, ysend, yrecv, zsend, zrecv, curved,
    arz, ary, arx,
    lsem, zs_s, zs_r, ys_s, ys_r, xr_s, xr_r, xl_s, xl_r, xf_s, xf_r, d_s, d_r,
    d2_s, d2_r, f2_s, f2_r, n2_s, l2_r, r2_r, y2_s, y2_r, z2_s, z2_r,
    az_s, az_r, ay_s, ay_r, ax_s, ax_r,
):
    dp = lax.axis_index("dp")
    mp = lax.axis_index("mp")
    c = lax.rem(dp, 2)
    x = lax.rem(dp // 2, 4)
    y = (dp // 8) * 2 + mp // 4
    yl = mp // 4
    z = lax.rem(mp, 4)
    oc = 1 - c

    def dev(xx, yy, zz, cc):
        return {"dp": ((yy // 2) * 4 + xx) * 2 + cc, "mp": lax.rem(yy, 2) * 4 + zz}

    def mod4(v):
        return lax.rem(v + 8, 4)

    def blk(xx, dy, cc):
        yy = mod4(y + dy)
        return (((yy // 2) * 4 + xx) * 2 + cc) * 2 + lax.rem(yy, 2)

    def rows(b):
        return pl.ds(pl.multiple_of(b * BLK, BLK), BLK)

    def rcopy(src, dst, ss, rs, device):
        return pltpu.make_async_remote_copy(
            src_ref=src, dst_ref=dst, send_sem=ss, recv_sem=rs, device_id=device, device_id_type=MESH
        )

    ld_basis = pltpu.make_async_copy(basis_hbm, basis, lsem.at[0])
    ld_act = pltpu.make_async_copy(act_hbm, act, lsem.at[1])
    ld_curv = pltpu.make_async_copy(curv_hbm, curv, lsem.at[2])
    ld_basis.start()
    ld_act.start()
    ld_curv.start()

    barrier = pltpu.get_barrier_semaphore()
    partners = [dev(x, y, z, oc)]
    for k in (1, 2, 3):
        partners.append(dev(x, y, mod4(z + k), c))
        partners.append(dev(x, y, mod4(z + k), oc))
        partners.append(dev(x, mod4(y + k), z, c))
        partners.append(dev(mod4(x + k), y, z, c))
    for p in partners:
        pl.semaphore_signal(barrier, inc=1, device_id=p, device_id_type=MESH)

    for h in range(8):
        for kv in range(2):
            v = kry_ref[pl.ds(2 * h + kv, 64, stride=16), :]
            ksend[h % 4, h // 4, :, kv * 128 : (kv + 1) * 128] = v.astype(BF16)
    b0 = blk(x, 0, c)
    zrow = pl.multiple_of(z * 64, 64)
    vrow = pl.multiple_of(b0 * BLK + z * 64, 64)
    vmat[pl.ds(vrow, 64), :] = ksend[z, yl]
    zoth[pl.ds(zrow, 64), :] = ksend[z, 1 - yl]
    acc[...] = jnp.zeros_like(acc)

    pl.semaphore_wait(barrier, len(partners))

    sends = []
    zrecvs = []
    for k in (2, 1, 3):
        zt = mod4(z + k)
        d = dev(x, y, zt, c)
        for q, (src, dst) in enumerate(
            (
                (ksend.at[zt, 1 - yl], zoth.at[pl.ds(zrow, 64), :]),
                (ksend.at[zt, yl], vmat.at[pl.ds(vrow, 64), :]),
            )
        ):
            cp = rcopy(src, dst, zs_s.at[q * 3 + k - 1], zs_r.at[q * 3 + k - 1], d)
            cp.start()
            sends.append(cp)
            zrecvs.append(cp)

    def gram_chunk(i, carry):
        top, bot = carry
        top, bot = list(top), list(bot)
        cols = pl.ds(pl.multiple_of(i * 128, 128), 128)
        a = basis[0:8, cols]
        b = basis[8:12, cols]
        for j in range(NB):
            row = a[j : j + 1] if j < 8 else b[j - 8 : j - 7]
            top[j] = top[j] + a * jnp.broadcast_to(row, (8, 128))
            bot[j] = bot[j] + b * jnp.broadcast_to(row, (4, 128))
        return tuple(top), tuple(bot)

    gram_state = (
        tuple(jnp.zeros((8, 128), F32) for _ in range(NB)),
        tuple(jnp.zeros((4, 128), F32) for _ in range(NB)),
    )

    ld_basis.wait()
    gram_state = lax.fori_loop(0, 1024, gram_chunk, gram_state)

    for cp in zrecvs:
        cp.wait_recv()

    def vblk(b):
        return vmat.at[rows(b), :]

    def mm1(b):
        def tile(m, _):
            r = pl.ds(pl.multiple_of(m * 256, 256), 256)
            acc[r, :] += jnp.dot(act[r, rows(b)], vmat[rows(b), :], preferred_element_type=F32)
            return 0

        lax.fori_loop(0, 4, tile, 0)

    xp, xm, xf = mod4(x + 1), mod4(x - 1), mod4(x + 2)

    def x_right(dy):
        b = blk(x, dy, c)
        return rcopy(vblk(b), vblk(b), xr_s.at[dy], xr_r.at[dy], dev(xp, y, z, c))

    def x_left(dy):
        b = blk(x, dy, c)
        return rcopy(vblk(b), vblk(b), xl_s.at[dy], xl_r.at[dy], dev(xm, y, z, c))

    def x_far(dy):
        odd = lax.rem(dy, 2)
        b = blk(mod4(x - 1 + 2 * odd), dy, c)
        return rcopy(vblk(b), vblk(b), xf_s.at[dy], xf_r.at[dy], dev(mod4(x + 1 - 2 * odd), y, z, c))

    def d2d(xo, dy):
        b = blk(mod4(x + xo), dy, c)
        return rcopy(vblk(b), vblk(b), d_s.at[xo * 4 + dy], d_r.at[xo * 4 + dy], dev(x, y, z, oc))

    def to_dy(i):
        return i + (i // 2) * (5 - 2 * i)

    ycps = {}
    for k in (2, 1, 3):
        src = vblk(b0) if k == 2 else zoth
        cp = rcopy(src, vblk(b0), ys_s.at[k], ys_r.at[4 - k], dev(x, mod4(y + k), z, c))
        cp.start()
        sends.append(cp)
        ycps[4 - k] = cp
    ld_act.wait()
    for i in range(4):
        dy = (0, 1, 3, 2)[i]
        if dy:
            ycps[dy].wait_recv()
        x_right(dy).start()
        x_left(dy).start()
        d2d(0, dy).start()
        mm1(blk(x, dy, c))

    def near(i, _):
        dy = to_dy(i)
        x_right(dy).wait_recv()
        d2d(3, dy).start()
        x_left(dy).wait_recv()
        x_far(dy).start()
        d2d(1, dy).start()
        mm1(blk(xm, dy, c))
        mm1(blk(xp, dy, c))
        d2d(0, dy).wait_recv()
        mm1(blk(x, dy, oc))
        return 0

    lax.fori_loop(0, 4, near, 0)

    def far(i, _):
        dy = to_dy(i)
        x_far(dy).wait_recv()
        d2d(2, dy).start()
        mm1(blk(xf, dy, c))
        for xo, xx in ((3, xm), (1, xp)):
            d2d(xo, dy).wait_recv()
            mm1(blk(xx, dy, oc))
        return 0

    lax.fori_loop(0, 4, far, 0)

    def last(i, _):
        dy = to_dy(i)
        d2d(2, dy).wait_recv()
        mm1(blk(xf, dy, oc))
        return 0

    lax.fori_loop(0, 4, last, 0)

    ld_curv.wait()
    for m in range(4):
        r = slice(m * 256, (m + 1) * 256)
        wt[:, r] = (curv[r, :] * acc[r, :]).T.astype(BF16)

    def mm2(b):
        return jnp.dot(wt[...], act[:, rows(b)], preferred_element_type=F32)

    def d2d2(i):
        return rcopy(dsend.at[i], drecv.at[i], d2_s.at[i], d2_r.at[i], dev(x, y, z, oc))

    def xo_of(i):
        return i

    def idx(xo, dy):
        return xo * 4 + dy

    def other(i, _):
        g = i // 4
        xo = lax.rem(2 + g * 3, 4)
        k = xo * 4 + lax.rem(i, 4)
        dsend[k] = mm2(blk(mod4(x + xo), lax.rem(i, 4), oc)).astype(BF16)
        d2d2(k).start()
        return 0

    lax.fori_loop(0, 16, other, 0)

    def chip_sum(xo, dy):
        k = idx(xo, dy)
        own = mm2(blk(mod4(x + xo), dy, c))
        d2d2(k).wait_recv()
        return own + drecv[k].astype(F32)

    def far2(dy):
        odd = lax.rem(dy, 2)
        return rcopy(xfs.at[dy], xfr.at[dy], f2_s.at[dy], f2_r.at[dy], dev(mod4(x - 1 + 2 * odd), y, z, c))

    def right2(dy):
        return rcopy(xns.at[dy], xl.at[dy], n2_s.at[dy], l2_r.at[dy], dev(xp, y, z, c))

    def left2(dy):
        return rcopy(xns.at[4 + dy], xr.at[dy], n2_s.at[4 + dy], r2_r.at[dy], dev(xm, y, z, c))

    def far_send(i, _):
        dy = to_dy(3 - i)
        xfs[dy] = chip_sum(2, dy).astype(BF16)
        far2(dy).start()
        return 0

    lax.fori_loop(0, 4, far_send, 0)

    def near_send(i, _):
        dy = to_dy(3 - i)
        odd = lax.rem(dy, 2)
        xo = 1 + 2 * odd
        xns[odd * 4 + dy] = chip_sum(xo, dy).astype(BF16)

        @pl.when(odd == 0)
        def _():
            right2(dy).start()

        @pl.when(odd == 1)
        def _():
            left2(dy).start()

        return 0

    lax.fori_loop(0, 4, near_send, 0)

    def near_add(i, _):
        dy = to_dy(3 - i)
        odd = lax.rem(dy, 2)
        xo = 3 - 2 * odd
        s = chip_sum(xo, dy)
        far2(dy).wait_recv()
        xns[(1 - odd) * 4 + dy] = (s + xfr[dy].astype(F32)).astype(BF16)

        @pl.when(odd == 0)
        def _():
            left2(dy).start()

        @pl.when(odd == 1)
        def _():
            right2(dy).start()

        return 0

    lax.fori_loop(0, 4, near_add, 0)

    def x_sum(dy):
        s = chip_sum(0, dy)
        right2(dy).wait_recv()
        left2(dy).wait_recv()
        return s + xl[dy].astype(F32) + xr[dy].astype(F32)

    def y2(k):
        return rcopy(ysend.at[k], yrecv.at[4 - k], y2_s.at[k], y2_r.at[4 - k], dev(x, mod4(y + k), z, c))

    for k in (2, 3, 1):
        ysend[k] = x_sum(k).astype(BF16)
        cp = y2(k)
        cp.start()
        sends.append(cp)
    h_own = x_sum(0)
    y2(1).wait_recv()
    y2(3).wait_recv()
    h_oth = yrecv[1].astype(F32) + yrecv[3].astype(F32)
    h_oth = h_oth.T.astype(BF16)
    for zz in range(4):
        zsend[zz, 1 - yl] = h_oth[zz * 64 : (zz + 1) * 64, :]
    y2(2).wait_recv()
    h_own = (h_own + yrecv[2].astype(F32)).T.astype(BF16)
    for zz in range(4):
        zsend[zz, yl] = h_own[zz * 64 : (zz + 1) * 64, :]

    zcps = []
    for k in (2, 1, 3):
        zt = mod4(z + k)
        cp = rcopy(zsend.at[zt], zrecv.at[z], z2_s.at[k - 1], z2_r.at[k - 1], dev(x, y, zt, c))
        cp.start()
        sends.append(cp)
        zcps.append(cp)
    zrecv[z] = zsend[z]
    for cp in zcps:
        cp.wait_recv()

    for zz in range(4):
        for hl in range(2):
            for kv in range(2):
                v = zrecv[zz, hl, :, kv * 128 : (kv + 1) * 128].astype(F32) * (1.0 / TOKENS)
                curved[pl.ds(2 * (hl * 4 + zz) + kv, 64, stride=16), :] = v

    def dot_chunk(i, carry):
        tops, bots, sq = carry
        tops, bots = list(tops), list(bots)
        t = curved[pl.ds(pl.multiple_of(i * 8, 8), 8), :]
        for s in range(8):
            cols = pl.ds(pl.multiple_of(i * 1024 + s * 128, 128), 128)
            row = t[s : s + 1]
            tops[s % 4] = tops[s % 4] + basis[0:8, cols] * jnp.broadcast_to(row, (8, 128))
            bots[s % 4] = bots[s % 4] + basis[8:12, cols] * jnp.broadcast_to(row, (4, 128))
        return tuple(tops), tuple(bots), sq + t * t

    tops, bots, sq = lax.fori_loop(
        0,
        128,
        dot_chunk,
        (
            tuple(jnp.zeros((8, 128), F32) for _ in range(4)),
            tuple(jnp.zeros((4, 128), F32) for _ in range(4)),
            jnp.zeros((8, 128), F32),
        ),
    )
    top = (tops[0] + tops[1]) + (tops[2] + tops[3])
    bot = (bots[0] + bots[1]) + (bots[2] + bots[3])

    lane8 = lax.broadcasted_iota(jnp.int32, (8, 128), 1)
    sub8 = lax.broadcasted_iota(jnp.int32, (8, 128), 0)
    zero4 = jnp.zeros((4, 128), F32)

    def lanes(v):
        return jnp.broadcast_to(jnp.sum(v, axis=1, keepdims=True), (8, 128))

    def pad(v):
        return jnp.concatenate([v, zero4], axis=0)

    up = jnp.where(lane8 == NB, lanes(top), 0.0)
    dn = jnp.where(lane8 == NB, lanes(pad(bot)), 0.0)
    for j in range(NB):
        up = jnp.where(lane8 == j, lanes(gram_state[0][j]), up)
        dn = jnp.where(lane8 == j, lanes(pad(gram_state[1][j])), dn)
    up = jnp.where(lane8 == NB + 1, lanes(sq), up)

    me = z * 2 + c
    arz[me, 0:8, :] = up
    arz[me, 8:16, :] = dn
    cps = []
    for k in range(1, 8):
        t = lax.rem(me + k, 8)
        cp = rcopy(
            arz.at[me], arz.at[me], az_s.at[k], az_r.at[k], dev(x, y, t // 2, lax.rem(t, 2))
        )
        cp.start()
        cps.append(cp)
    for cp in cps:
        cp.wait_recv()
    sends += cps
    tot = arz[0]
    for k in range(1, 8):
        tot = tot + arz[k]
    for buf, me, ss, rs, axis in ((ary, y, ay_s, ay_r, 0), (arx, x, ax_s, ax_r, 1)):
        buf[me] = tot
        cps = []
        for k in (2, 1, 3):
            t = mod4(me + k)
            d = dev(x, t, z, c) if axis == 0 else dev(t, y, z, c)
            cp = rcopy(buf.at[me], buf.at[me], ss.at[k], rs.at[k], d)
            cp.start()
            cps.append(cp)
        for cp in cps:
            cp.wait_recv()
        sends += cps
        tot = (buf[0] + buf[1]) + (buf[2] + buf[3])

    tot = tot * (1.0 / PARAMS)
    gt, gb = tot[0:8], tot[8:16]

    def pick(v, lane):
        return lanes(jnp.where(lane8 == lane, v, 0.0))

    ct, cb = pick(gt, NB), pick(gb, NB)
    crow = jnp.sum(
        jnp.where(lane8 == sub8, ct, 0.0) + jnp.where(lane8 == sub8 + 8, cb, 0.0), axis=0, keepdims=True
    )
    gc = jnp.sum(gt * ct + gb * cb, axis=0, keepdims=True)
    cgc = jnp.sum(crow * gc, axis=1, keepdims=True)
    cc = jnp.sum(crow * crow, axis=1, keepdims=True)
    squares = jnp.sum(jnp.where(lane8 == NB + 1, gt, 0.0), axis=0, keepdims=True)
    squares = jnp.sum(squares, axis=1, keepdims=True)
    norm = jnp.sqrt(squares - 2.0 * cc + cgc + 1e-06)
    inv = jnp.broadcast_to(1.0 / norm, (8, 128))
    lane1 = lax.broadcasted_iota(jnp.int32, (1, 128), 1)
    hess_ref[...] = jnp.where(lane1 == NB, jnp.broadcast_to(norm, (1, 128)), crow)

    def res_chunk(i, _):
        t = []
        for s in range(8):
            cols = pl.ds(pl.multiple_of(i * 1024 + s * 128, 128), 128)
            t.append(basis[0:8, cols] * ct + pad(basis[8:12, cols]) * cb)
        for sh in (4, 2, 1):
            keep = lax.rem(sub8 // sh, 2) == 0
            t = [
                jnp.where(
                    keep,
                    t[s] + pltpu.roll(t[s], 8 - sh, 0),
                    t[s + sh] + pltpu.roll(t[s + sh], sh, 0),
                )
                for s in range(sh)
            ]
        r = pl.ds(pl.multiple_of(i * 8, 8), 8)
        out_ref[r, :] = (curved[r, :] - t[0]) * inv
        return 0

    lax.fori_loop(0, 128, res_chunk, 0)

    for cp in sends:
        cp.wait_send()

    def drain(dy, _):
        x_right(dy).wait_send()
        x_left(dy).wait_send()
        x_far(dy).wait_send()
        far2(dy).wait_send()
        right2(dy).wait_send()
        left2(dy).wait_send()
        for xo in range(4):
            d2d(xo, dy).wait_send()
            d2d2(xo * 4 + dy).wait_send()
        return 0

    lax.fori_loop(0, 4, drain, 0)


def body(activations, curvature, basis, krylov):
    dma = pltpu.SemaphoreType.DMA
    vm = pltpu.VMEM
    anyspace = pl.BlockSpec(memory_space=pl.ANY)
    vspace = pl.BlockSpec(memory_space=pltpu.VMEM)
    blocks = lambda n: vm((n, 256, 256), BF16)
    out, hess = pl.pallas_call(
        kernel,
        out_shape=(jax.ShapeDtypeStruct((1024, 128), F32), jax.ShapeDtypeStruct((1, 128), F32)),
        in_specs=[anyspace, anyspace, anyspace, vspace],
        out_specs=(vspace, vspace),
        scratch_shapes=[
            vm((1024, 8192), BF16),
            vm((1024, 256), F32),
            vm((NB, 131072), F32),
            vm((8192, 256), BF16),
            vm((4, 2, 64, 256), BF16),
            vm((256, 256), BF16),
            vm((1024, 256), F32),
            vm((256, 1024), BF16),
            blocks(16),
            blocks(16),
            blocks(4),
            blocks(8),
            blocks(4),
            blocks(4),
            blocks(4),
            blocks(4),
            blocks(4),
            vm((4, 2, 64, 256), BF16),
            vm((4, 2, 64, 256), BF16),
            vm((1024, 128), F32),
            vm((8, 16, 128), F32),
            vm((4, 16, 128), F32),
            vm((4, 16, 128), F32),
            dma((3,)),
            dma((6,)),
            dma((6,)),
            dma((4,)),
            dma((4,)),
            dma((4,)),
            dma((4,)),
            dma((4,)),
            dma((4,)),
            dma((4,)),
            dma((4,)),
            dma((16,)),
            dma((16,)),
            dma((16,)),
            dma((16,)),
            dma((4,)),
            dma((4,)),
            dma((8,)),
            dma((4,)),
            dma((4,)),
            dma((4,)),
            dma((4,)),
            dma((3,)),
            dma((3,)),
            dma((8,)),
            dma((8,)),
            dma((4,)),
            dma((4,)),
            dma((4,)),
            dma((4,)),
        ],
        compiler_params=pltpu.CompilerParams(
            collective_id=0, has_side_effects=True, vmem_limit_bytes=63 * 1024 * 1024
        ),
    )(activations, curvature, basis, krylov.reshape(1024, 128))
    return out.reshape(131072), hess[0, :13]


def solution(mesh):
    placed = (P("dp", None), P("dp", "mp"), P(None, ("dp", "mp")), P(("dp", "mp")))
    return jax.shard_map(
        body, mesh=mesh, in_specs=placed, out_specs=(P(("dp", "mp")), P()), check_vma=False
    )
```

```python
import functools

import jax
import jax.numpy as jnp
from jax import lax
from jax.experimental import pallas as pl
from jax.experimental.pallas import tpu as pltpu
from jax.sharding import PartitionSpec as P

MESH = pl.DeviceIdType.MESH
TOKENS = 16384
PARAMS = 16777216
NB = 12
F32 = jnp.float32
BF16 = jnp.bfloat16
GRAM_UNROLL = 4
VMEM_MIB = 46
GRAM_PIECES = 8
BLK = 256


def kernel(
    act_hbm, curv, basis_hbm, kry_ref, out_ref, hess_ref,
    act, basis, vmat, ksend, zoth, acc, wt,
    dsend, drecv, xfs, xns, xfr, xl, xr, ysend, yrecv, zsend, zrecv, curved,
    arz, ary, arx, crz, cry, crx,
    lsem, zs_s, zs_r, ys_s, ys_r, xr_s, xr_r, xl_s, xl_r, xf_s, xf_r, d_s, d_r,
    d2_s, d2_r, f2_s, f2_r, n2_s, l2_r, r2_r, y2_s, y2_r, z2_s, z2_r,
    az_s, az_r, ay_s, ay_r, ax_s, ax_r, cz_s, cz_r, cy_s, cy_r, cx_s, cx_r,
):
    dp = lax.axis_index("dp")
    mp = lax.axis_index("mp")
    c = lax.rem(dp, 2)
    x = lax.rem(dp // 2, 4)
    y = (dp // 8) * 2 + mp // 4
    yl = mp // 4
    z = lax.rem(mp, 4)
    oc = 1 - c

    def dev(xx, yy, zz, cc):
        return {"dp": ((yy // 2) * 4 + xx) * 2 + cc, "mp": lax.rem(yy, 2) * 4 + zz}

    def mod4(v):
        return lax.rem(v + 8, 4)

    def blk(xx, dy, cc):
        yy = mod4(y + dy)
        return (((yy // 2) * 4 + xx) * 2 + cc) * 2 + lax.rem(yy, 2)

    def rows(b):
        return pl.ds(pl.multiple_of(b * BLK, BLK), BLK)

    def rcopy(src, dst, ss, rs, device):
        return pltpu.make_async_remote_copy(
            src_ref=src, dst_ref=dst, send_sem=ss, recv_sem=rs, device_id=device, device_id_type=MESH
        )

    ld_basis = pltpu.make_async_copy(basis_hbm, basis, lsem.at[0])
    ld_act = pltpu.make_async_copy(act_hbm, act, lsem.at[1])
    ld_basis.start()
    ld_act.start()
    barrier = pltpu.get_barrier_semaphore()
    partners = [dev(x, y, z, oc)]
    for k in (1, 2, 3):
        partners.append(dev(x, y, mod4(z + k), c))
        partners.append(dev(x, y, mod4(z + k), oc))
        partners.append(dev(x, mod4(y + k), z, c))
        partners.append(dev(mod4(x + k), y, z, c))
    for p in partners:
        pl.semaphore_signal(barrier, inc=1, device_id=p, device_id_type=MESH)

    for h in range(8):
        for kv in range(2):
            v = kry_ref[pl.ds(2 * h + kv, 64, stride=16), :]
            ksend[h % 4, h // 4, :, kv * 128 : (kv + 1) * 128] = v.astype(BF16)
    b0 = blk(x, 0, c)
    zrow = pl.multiple_of(z * 64, 64)
    vrow = pl.multiple_of(b0 * BLK + z * 64, 64)
    vmat[pl.ds(vrow, 64), :] = ksend[z, yl]
    zoth[pl.ds(zrow, 64), :] = ksend[z, 1 - yl]
    acc[...] = jnp.zeros_like(acc)

    pl.semaphore_wait(barrier, len(partners))

    sends = []
    zrecvs = ([], [])
    for q in range(2):
        for k in (2, 1, 3):
            zt = mod4(z + k)
            if q == 0:
                src, dst = ksend.at[zt, 1 - yl], zoth.at[pl.ds(zrow, 64), :]
            else:
                src, dst = ksend.at[zt, yl], vmat.at[pl.ds(vrow, 64), :]
            n = q * 3 + k - 1
            cp = rcopy(src, dst, zs_s.at[n], zs_r.at[n], dev(x, y, zt, c))
            cp.start()
            sends.append(cp)
            zrecvs[q].append(cp)

    def gram_chunk(i, carry):
        top, bot = carry
        top, bot = list(top), list(bot)
        for u in range(GRAM_UNROLL):
            cols = pl.ds(pl.multiple_of(i * (128 * GRAM_UNROLL) + u * 128, 128), 128)
            a = basis[0:8, cols]
            b = basis[8:12, cols]
            for j in range(NB):
                row = a[j : j + 1] if j < 8 else b[j - 8 : j - 7]
                top[j] = top[j] + a * jnp.broadcast_to(row, (8, 128))
                bot[j] = bot[j] + b * jnp.broadcast_to(row, (4, 128))
        return tuple(top), tuple(bot)

    gram_state = [
        (
            tuple(jnp.zeros((8, 128), F32) for _ in range(NB)),
            tuple(jnp.zeros((4, 128), F32) for _ in range(NB)),
        )
    ]
    steps = 1024 // GRAM_UNROLL // GRAM_PIECES
    done = [0]

    def gram():
        n = done[0]
        gram_state[0] = lax.fori_loop(n * steps, (n + 1) * steps, gram_chunk, gram_state[0])
        done[0] = n + 1

    def vblk(b):
        return vmat.at[rows(b), :]

    def mm1(bs):
        for m in range(2):
            r = slice(m * 512, (m + 1) * 512)
            p = [jnp.dot(act[r, rows(b)], vmat[rows(b), :], preferred_element_type=F32) for b in bs]
            acc[r, :] += functools.reduce(jnp.add, p)

    xp, xm, xf = mod4(x + 1), mod4(x - 1), mod4(x + 2)

    def x_right(dy):
        b = blk(x, dy, c)
        return rcopy(vblk(b), vblk(b), xr_s.at[dy], xr_r.at[dy], dev(xp, y, z, c))

    def x_left(dy):
        b = blk(x, dy, c)
        return rcopy(vblk(b), vblk(b), xl_s.at[dy], xl_r.at[dy], dev(xm, y, z, c))

    def x_far(dy):
        odd = lax.rem(dy, 2)
        b = blk(mod4(x - 1 + 2 * odd), dy, c)
        return rcopy(vblk(b), vblk(b), xf_s.at[dy], xf_r.at[dy], dev(mod4(x + 1 - 2 * odd), y, z, c))

    def d2d(xo, dy):
        b = blk(mod4(x + xo), dy, c)
        return rcopy(vblk(b), vblk(b), d_s.at[xo * 4 + dy], d_r.at[xo * 4 + dy], dev(x, y, z, oc))

    def to_dy(i):
        return i + (i // 2) * (5 - 2 * i)

    ld_basis.wait()
    gram()

    ycps = {}

    def y_send(k):
        src = vblk(b0) if k == 2 else zoth
        cp = rcopy(src, vblk(b0), ys_s.at[k], ys_r.at[4 - k], dev(x, mod4(y + k), z, c))
        cp.start()
        sends.append(cp)
        ycps[4 - k] = cp

    def own_block(dy):
        x_right(dy).start()
        x_left(dy).start()
        d2d(0, dy).start()

    def ring(dy):
        x_right(dy).wait_recv()
        x_left(dy).wait_recv()
        x_far(dy).start()
        d2d(3, dy).start()
        d2d(1, dy).start()

    def mine(*which):
        mm1([blk(xx, dy, c) for xx, dy in which])

    def others(*which):
        for xo, dy in which:
            d2d(xo, dy).wait_recv()
        mm1([blk(mod4(x + xo), dy, oc) for xo, dy in which])

    for cp in zrecvs[0]:
        cp.wait_recv()
    y_send(1)
    y_send(3)
    for cp in zrecvs[1]:
        cp.wait_recv()
    own_block(0)
    y_send(2)
    gram()
    ld_act.wait()
    mine((x, 0))
    ycps[1].wait_recv()
    own_block(1)
    ycps[3].wait_recv()
    own_block(3)
    ring(0)
    gram()
    mine((x, 1), (x, 3))
    ring(1)
    mine((xm, 0), (xp, 0))
    ycps[2].wait_recv()
    own_block(2)
    gram()
    others((0, 0), (0, 1))
    ring(3)
    mine((xm, 1), (xp, 1))
    gram()
    ring(2)
    mine((x, 2))
    gram()
    others((0, 3), (3, 0), (1, 0))
    x_far(0).wait_recv()
    d2d(2, 0).start()
    mine((xm, 3), (xp, 3), (xm, 2), (xp, 2))
    x_far(1).wait_recv()
    d2d(2, 1).start()
    gram()
    mine((xf, 0), (xf, 1))
    others((3, 1), (1, 1), (0, 2), (2, 0))
    x_far(3).wait_recv()
    d2d(2, 3).start()
    mine((xf, 3))
    gram()
    others((3, 3), (1, 3), (3, 2), (1, 2), (2, 1))
    x_far(2).wait_recv()
    d2d(2, 2).start()
    mine((xf, 2))
    others((2, 3), (2, 2))
    gram_state = gram_state[0]

    lane8 = lax.broadcasted_iota(jnp.int32, (8, 128), 1)
    sub8 = lax.broadcasted_iota(jnp.int32, (8, 128), 0)
    zero4 = jnp.zeros((4, 128), F32)

    def lanes(v):
        return jnp.broadcast_to(jnp.sum(v, axis=1, keepdims=True), (8, 128))

    def pad(v):
        return jnp.concatenate([v, zero4], axis=0)

    def reduce_start(stage, buf, value, ss, rs):
        me, count = ((z * 2 + c, 8), (y, 4), (x, 4))[stage]
        buf[me] = value
        cps = []
        for k in range(1, count):
            t = lax.rem(me + k, count)
            d = (
                dev(x, y, t // 2, lax.rem(t, 2)) if stage == 0 else dev(x, t, z, c) if stage == 1 else dev(t, y, z, c)
            )
            cp = rcopy(buf.at[me], buf.at[me], ss.at[k], rs.at[k], d)
            cp.start()
            cps.append(cp)
        sends.extend(cps)
        return cps, buf, count

    def reduce_end(started):
        cps, buf, count = started
        for cp in cps:
            cp.wait_recv()
        parts = [buf[k] for k in range(count)]
        while len(parts) > 1:
            parts = [parts[k] + parts[k + 1] for k in range(0, len(parts), 2)]
        return parts[0]

    gup = jnp.zeros((8, 128), F32)
    gdn = jnp.zeros((8, 128), F32)
    for j in range(NB):
        gup = jnp.where(lane8 == j, lanes(gram_state[0][j]), gup)
        gdn = jnp.where(lane8 == j, lanes(pad(gram_state[1][j])), gdn)
    gram_sum = reduce_start(0, arz, jnp.concatenate([gup, gdn], axis=0), az_s, az_r)


    for m in range(4):
        r = slice(m * 256, (m + 1) * 256)
        wt[:, r] = (curv[r, :] * acc[r, :]).T.astype(BF16)

    def mm2(b):
        return jnp.dot(wt[...], act[:, rows(b)], preferred_element_type=F32)

    def d2d2(i):
        return rcopy(dsend.at[i], drecv.at[i], d2_s.at[i], d2_r.at[i], dev(x, y, z, oc))

    def idx(xo, dy):
        return xo * 4 + dy

    def other(*which):
        ps = [mm2(blk(mod4(x + xo), dy, oc)).astype(BF16) for xo, dy in which]
        for (xo, dy), p in zip(which, ps):
            dsend[idx(xo, dy)] = p
        for xo, dy in which:
            d2d2(idx(xo, dy)).start()

    def chip_sums(*which):
        ps = [mm2(blk(mod4(x + xo), dy, c)) for xo, dy in which]
        for xo, dy in which:
            d2d2(idx(xo, dy)).wait_recv()
        return [p + drecv[idx(xo, dy)].astype(F32) for (xo, dy), p in zip(which, ps)]

    def far2(dy):
        odd = lax.rem(dy, 2)
        return rcopy(xfs.at[dy], xfr.at[dy], f2_s.at[dy], f2_r.at[dy], dev(mod4(x - 1 + 2 * odd), y, z, c))

    def right2(dy):
        return rcopy(xns.at[dy], xl.at[dy], n2_s.at[dy], l2_r.at[dy], dev(xp, y, z, c))

    def left2(dy):
        return rcopy(xns.at[4 + dy], xr.at[dy], n2_s.at[4 + dy], r2_r.at[dy], dev(xm, y, z, c))

    def far_send(*dys):
        for dy, s in zip(dys, chip_sums(*((2, dy) for dy in dys))):
            xfs[dy] = s.astype(BF16)
        for dy in dys:
            far2(dy).start()

    def near_send(*dys):
        for dy, s in zip(dys, chip_sums(*((1 + 2 * (dy % 2), dy) for dy in dys))):
            xns[(dy % 2) * 4 + dy] = s.astype(BF16)
        for dy in dys:
            (left2 if dy % 2 else right2)(dy).start()

    def near_add(*dys):
        sums = chip_sums(*((3 - 2 * (dy % 2), dy) for dy in dys))
        for dy in dys:
            far2(dy).wait_recv()
        for dy, s in zip(dys, sums):
            xns[(1 - dy % 2) * 4 + dy] = (s + xfr[dy].astype(F32)).astype(BF16)
        for dy in dys:
            (right2 if dy % 2 else left2)(dy).start()

    early, late = (2, 3), (1, 0)
    other((2, 2), (2, 3))
    other((2, 1), (2, 0))
    other((1, 2), (3, 3))
    far_send(*early)
    far_send(*late)
    other((3, 1), (1, 0))
    near_send(*early)
    other((3, 2), (1, 3))
    near_send(*late)
    other((1, 1), (3, 0))
    gram_sum = reduce_start(1, ary, reduce_end(gram_sum), ay_s, ay_r)
    near_add(*early)
    other((0, 2), (0, 3))
    near_add(*late)
    other((0, 1), (0, 0))
    gram_sum = reduce_start(2, arx, reduce_end(gram_sum), ax_s, ax_r)
    x_own = dict(zip((2, 3, 1, 0), chip_sums((0, 2), (0, 3), (0, 1), (0, 0))))

    def x_sum(dy):
        right2(dy).wait_recv()
        left2(dy).wait_recv()
        return x_own[dy] + xl[dy].astype(F32) + xr[dy].astype(F32)

    def y2(k):
        return rcopy(ysend.at[k], yrecv.at[4 - k], y2_s.at[k], y2_r.at[4 - k], dev(x, mod4(y + k), z, c))

    for k in (2, 3, 1):
        ysend[k] = x_sum(k).astype(BF16)
        cp = y2(k)
        cp.start()
        sends.append(cp)
    h_own = x_sum(0)
    y2(1).wait_recv()
    y2(3).wait_recv()
    h_oth = yrecv[1].astype(F32) + yrecv[3].astype(F32)
    zcps = []

    def z2(value, head, q):
        v = value.T.astype(BF16)
        for zz in range(4):
            zsend[zz, head] = v[zz * 64 : (zz + 1) * 64, :]
        for k in (2, 1, 3):
            zt = mod4(z + k)
            n = q * 3 + k - 1
            cp = rcopy(zsend.at[zt, head], zrecv.at[z, head], z2_s.at[n], z2_r.at[n], dev(x, y, zt, c))
            cp.start()
            sends.append(cp)
            zcps.append(cp)

    z2(h_oth, 1 - yl, 0)
    y2(2).wait_recv()
    z2(h_own + yrecv[2].astype(F32), yl, 1)
    zrecv[z] = zsend[z]
    for cp in zcps:
        cp.wait_recv()

    for zz in range(4):
        for hl in range(2):
            for kv in range(2):
                v = zrecv[zz, hl, :, kv * 128 : (kv + 1) * 128].astype(F32) * (1.0 / TOKENS)
                curved[pl.ds(2 * (hl * 4 + zz) + kv, 64, stride=16), :] = v

    def dot_chunk(i, carry):
        tops, bots, sq = carry
        tops, bots = list(tops), list(bots)
        for u in range(4):
            t = curved[pl.ds(pl.multiple_of(i * 32 + u * 8, 8), 8), :]
            sq = sq + t * t
            for s in range(8):
                cols = pl.ds(pl.multiple_of(i * 4096 + u * 1024 + s * 128, 128), 128)
                row = t[s : s + 1]
                tops[s % 4] = tops[s % 4] + basis[0:8, cols] * jnp.broadcast_to(row, (8, 128))
                bots[s % 4] = bots[s % 4] + basis[8:12, cols] * jnp.broadcast_to(row, (4, 128))
        return tuple(tops), tuple(bots), sq

    tops, bots, sq = lax.fori_loop(
        0,
        32,
        dot_chunk,
        (
            tuple(jnp.zeros((8, 128), F32) for _ in range(4)),
            tuple(jnp.zeros((4, 128), F32) for _ in range(4)),
            jnp.zeros((8, 128), F32),
        ),
    )
    top = (tops[0] + tops[1]) + (tops[2] + tops[3])
    bot = (bots[0] + bots[1]) + (bots[2] + bots[3])

    row = jnp.sum(
        jnp.where(lane8 == sub8, lanes(top), 0.0)
        + jnp.where(lane8 == sub8 + 8, lanes(pad(bot)), 0.0)
        + jnp.where(lane8 == NB, lanes(sq), 0.0),
        axis=0,
        keepdims=True,
    )
    row = reduce_end(reduce_start(0, crz, row, cz_s, cz_r))
    row = reduce_end(reduce_start(1, cry, row, cy_s, cy_r))
    row = reduce_end(reduce_start(2, crx, row, cx_s, cx_r))
    row = row * (1.0 / PARAMS)
    tot = reduce_end(gram_sum) * (1.0 / PARAMS)
    gt, gb = tot[0:8], tot[8:16]
    lane1 = lax.broadcasted_iota(jnp.int32, (1, 128), 1)
    crow = jnp.where(lane1 < NB, row, 0.0)
    ct = lanes(jnp.where(lane8 == sub8, jnp.broadcast_to(crow, (8, 128)), 0.0))
    cb = lanes(jnp.where(lane8 == sub8 + 8, jnp.broadcast_to(crow, (8, 128)), 0.0))
    gc = jnp.sum(gt * ct + gb * cb, axis=0, keepdims=True)
    cgc = jnp.sum(crow * gc, axis=1, keepdims=True)
    cc = jnp.sum(crow * crow, axis=1, keepdims=True)
    squares = jnp.sum(jnp.where(lane1 == NB, row, 0.0), axis=1, keepdims=True)
    norm = jnp.sqrt(squares - 2.0 * cc + cgc + 1e-06)
    inv = jnp.broadcast_to(1.0 / norm, (8, 128))
    hess_ref[...] = jnp.where(lane1 == NB, jnp.broadcast_to(norm, (1, 128)), crow)

    def res_chunk(i, _):
        for u in range(4):
            t = []
            for s in range(8):
                cols = pl.ds(pl.multiple_of(i * 4096 + u * 1024 + s * 128, 128), 128)
                t.append(basis[0:8, cols] * ct + pad(basis[8:12, cols]) * cb)
            for sh in (4, 2, 1):
                keep = lax.rem(sub8 // sh, 2) == 0
                t = [
                    jnp.where(
                        keep,
                        t[s] + pltpu.roll(t[s], 8 - sh, 0),
                        t[s + sh] + pltpu.roll(t[s + sh], sh, 0),
                    )
                    for s in range(sh)
                ]
            r = pl.ds(pl.multiple_of(i * 32 + u * 8, 8), 8)
            out_ref[r, :] = (curved[r, :] - t[0]) * inv
        return 0

    lax.fori_loop(0, 32, res_chunk, 0)

    for cp in sends:
        cp.wait_send()

    def drain(dy, _):
        x_right(dy).wait_send()
        x_left(dy).wait_send()
        x_far(dy).wait_send()
        far2(dy).wait_send()
        right2(dy).wait_send()
        left2(dy).wait_send()
        for xo in range(4):
            d2d(xo, dy).wait_send()
            d2d2(xo * 4 + dy).wait_send()
        return 0

    lax.fori_loop(0, 4, drain, 0)


def body(activations, curvature, basis, krylov):
    dma = pltpu.SemaphoreType.DMA
    vm = pltpu.VMEM
    anyspace = pl.BlockSpec(memory_space=pltpu.HBM)
    vspace = pl.BlockSpec(memory_space=pltpu.VMEM)
    blocks = lambda n: vm((n, 256, 256), BF16)
    out, hess = pl.pallas_call(
        kernel,
        out_shape=(jax.ShapeDtypeStruct((1024, 128), F32), jax.ShapeDtypeStruct((1, 128), F32)),
        in_specs=[anyspace, vspace, anyspace, vspace],
        out_specs=(vspace, vspace),
        scratch_shapes=[
            vm((1024, 8192), BF16),
            vm((NB, 131072), F32),
            vm((8192, 256), BF16),
            vm((4, 2, 64, 256), BF16),
            vm((256, 256), BF16),
            vm((1024, 256), F32),
            vm((256, 1024), BF16),
            blocks(16),
            blocks(16),
            blocks(4),
            blocks(8),
            blocks(4),
            blocks(4),
            blocks(4),
            blocks(4),
            blocks(4),
            vm((4, 2, 64, 256), BF16),
            vm((4, 2, 64, 256), BF16),
            vm((1024, 128), F32),
            vm((8, 16, 128), F32),
            vm((4, 16, 128), F32),
            vm((4, 16, 128), F32),
            vm((8, 1, 128), F32),
            vm((4, 1, 128), F32),
            vm((4, 1, 128), F32),
            dma((3,)),
            dma((6,)),
            dma((6,)),
            dma((4,)),
            dma((4,)),
            dma((4,)),
            dma((4,)),
            dma((4,)),
            dma((4,)),
            dma((4,)),
            dma((4,)),
            dma((16,)),
            dma((16,)),
            dma((16,)),
            dma((16,)),
            dma((4,)),
            dma((4,)),
            dma((8,)),
            dma((4,)),
            dma((4,)),
            dma((4,)),
            dma((4,)),
            dma((6,)),
            dma((6,)),
            dma((8,)),
            dma((8,)),
            dma((4,)),
            dma((4,)),
            dma((4,)),
            dma((4,)),
            dma((8,)),
            dma((8,)),
            dma((4,)),
            dma((4,)),
            dma((4,)),
            dma((4,)),
        ],
        compiler_params=pltpu.CompilerParams(
            collective_id=0, has_side_effects=True, vmem_limit_bytes=VMEM_MIB * 1024 * 1024
        ),
    )(activations, curvature, basis, krylov.reshape(1024, 128))
    return out.reshape(131072), hess[0, :13]


def solution(mesh):
    placed = (P("dp", None), P("dp", "mp"), P(None, ("dp", "mp")), P(("dp", "mp")))
    return jax.shard_map(
        body, mesh=mesh, in_specs=placed, out_specs=(P(("dp", "mp")), P()), check_vma=False
    )
```

```python
import functools

import jax
import jax.numpy as jnp
from jax import lax
from jax.experimental import pallas as pl
from jax.experimental.pallas import tpu as pltpu
from jax.sharding import PartitionSpec as P

MESH = pl.DeviceIdType.MESH
TOKENS = 16384
PARAMS = 16777216
NB = 12
F32 = jnp.float32
BF16 = jnp.bfloat16
GRAM_UNROLL = 4
VMEM_BYTES = 55_750_000
GRAM_PIECES = 8
BLK = 256


def kernel(
    act_hbm, curv_hbm, basis_hbm, kry_hbm, out_ref, hess_ref,
    act, curv, basis, kry_ref, vmat, ksend, zoth, acc, wt,
    dsend, drecv, xfs, xns, xfr, xl, xr, ysend, yrecv, zsend, zrecv, curved,
    arz, ary, arx, crz, cry, crx,
    lsem, zs_s, zs_r, ys_s, ys_r, xr_s, xr_r, xl_s, xl_r, xf_s, xf_r, d_s, d_r,
    d2_s, d2_r, f2_s, f2_r, n2_s, l2_r, r2_r, y2_s, y2_r, z2_s, z2_r,
    az_s, az_r, ay_s, ay_r, ax_s, ax_r, cz_s, cz_r, cy_s, cy_r, cx_s, cx_r,
):
    dp = lax.axis_index("dp")
    mp = lax.axis_index("mp")
    c = lax.rem(dp, 2)
    x = lax.rem(dp // 2, 4)
    y = (dp // 8) * 2 + mp // 4
    yl = mp // 4
    z = lax.rem(mp, 4)
    oc = 1 - c

    def dev(xx, yy, zz, cc):
        return {"dp": ((yy // 2) * 4 + xx) * 2 + cc, "mp": lax.rem(yy, 2) * 4 + zz}

    def mod4(v):
        return lax.rem(v + 8, 4)

    def blk(xx, dy, cc):
        yy = mod4(y + dy)
        return (((yy // 2) * 4 + xx) * 2 + cc) * 2 + lax.rem(yy, 2)

    def rows(b):
        return pl.ds(pl.multiple_of(b * BLK, BLK), BLK)

    def rcopy(src, dst, ss, rs, device):
        return pltpu.make_async_remote_copy(
            src_ref=src, dst_ref=dst, send_sem=ss, recv_sem=rs, device_id=device, device_id_type=MESH
        )

    first, rest = pl.ds(0, 32768), pl.ds(32768, 98304)
    ld_basis = pltpu.make_async_copy(basis_hbm.at[:, first], basis.at[:, first], lsem.at[0])
    ld_rest = pltpu.make_async_copy(basis_hbm.at[:, rest], basis.at[:, rest], lsem.at[4])
    ld_act = pltpu.make_async_copy(act_hbm, act, lsem.at[1])
    ld_curv = pltpu.make_async_copy(curv_hbm, curv, lsem.at[2])
    ld_kry = pltpu.make_async_copy(kry_hbm, kry_ref, lsem.at[3])
    ld_kry.start()
    ld_basis.start()
    ld_act.start()
    ld_rest.start()
    ld_curv.start()

    barrier = pltpu.get_barrier_semaphore()
    partners = [dev(x, y, z, oc)]
    for k in (1, 2, 3):
        partners.append(dev(x, y, mod4(z + k), c))
        partners.append(dev(x, y, mod4(z + k), oc))
        partners.append(dev(x, mod4(y + k), z, c))
        partners.append(dev(mod4(x + k), y, z, c))
    for p in partners:
        pl.semaphore_signal(barrier, inc=1, device_id=p, device_id_type=MESH)

    acc[...] = jnp.zeros_like(acc)
    ld_kry.wait()

    for h in range(8):
        for kv in range(2):
            v = kry_ref[pl.ds(2 * h + kv, 64, stride=16), :]
            ksend[h % 4, h // 4, :, kv * 128 : (kv + 1) * 128] = v.astype(BF16)
    b0 = blk(x, 0, c)
    zrow = pl.multiple_of(z * 64, 64)
    vrow = pl.multiple_of(b0 * BLK + z * 64, 64)
    vmat[pl.ds(vrow, 64), :] = ksend[z, yl]
    zoth[pl.ds(zrow, 64), :] = ksend[z, 1 - yl]

    pl.semaphore_wait(barrier, len(partners))

    sends = []
    zrecvs = ([], [])
    for q in range(2):
        for k in (2, 1, 3):
            zt = mod4(z + k)
            if q == 0:
                src, dst = ksend.at[zt, 1 - yl], zoth.at[pl.ds(zrow, 64), :]
            else:
                src, dst = ksend.at[zt, yl], vmat.at[pl.ds(vrow, 64), :]
            n = q * 3 + k - 1
            cp = rcopy(src, dst, zs_s.at[n], zs_r.at[n], dev(x, y, zt, c))
            cp.start()
            sends.append(cp)
            zrecvs[q].append(cp)

    def gram_chunk(i, carry):
        top, bot = carry
        top, bot = list(top), list(bot)
        for u in range(GRAM_UNROLL):
            cols = pl.ds(pl.multiple_of(i * (128 * GRAM_UNROLL) + u * 128, 128), 128)
            a = basis[0:8, cols]
            b = basis[8:12, cols]
            for j in range(NB):
                row = a[j : j + 1] if j < 8 else b[j - 8 : j - 7]
                top[j] = top[j] + a * jnp.broadcast_to(row, (8, 128))
                bot[j] = bot[j] + b * jnp.broadcast_to(row, (4, 128))
        return tuple(top), tuple(bot)

    gram_state = [
        (
            tuple(jnp.zeros((8, 128), F32) for _ in range(NB)),
            tuple(jnp.zeros((4, 128), F32) for _ in range(NB)),
        )
    ]
    steps = 1024 // GRAM_UNROLL // GRAM_PIECES
    done = [0]

    def gram():
        n = done[0]
        gram_state[0] = lax.fori_loop(n * steps, (n + 1) * steps, gram_chunk, gram_state[0])
        done[0] = n + 1

    def vblk(b):
        return vmat.at[rows(b), :]

    def mm1(bs):
        for m in range(2):
            r = slice(m * 512, (m + 1) * 512)
            p = [jnp.dot(act[r, rows(b)], vmat[rows(b), :], preferred_element_type=F32) for b in bs]
            acc[r, :] += functools.reduce(jnp.add, p)

    xp, xm, xf = mod4(x + 1), mod4(x - 1), mod4(x + 2)

    def x_right(dy):
        b = blk(x, dy, c)
        return rcopy(vblk(b), vblk(b), xr_s.at[dy], xr_r.at[dy], dev(xp, y, z, c))

    def x_left(dy):
        b = blk(x, dy, c)
        return rcopy(vblk(b), vblk(b), xl_s.at[dy], xl_r.at[dy], dev(xm, y, z, c))

    def x_far(dy):
        odd = lax.rem(dy, 2)
        b = blk(mod4(x - 1 + 2 * odd), dy, c)
        return rcopy(vblk(b), vblk(b), xf_s.at[dy], xf_r.at[dy], dev(mod4(x + 1 - 2 * odd), y, z, c))

    def d2d(xo, dy):
        b = blk(mod4(x + xo), dy, c)
        return rcopy(vblk(b), vblk(b), d_s.at[xo * 4 + dy], d_r.at[xo * 4 + dy], dev(x, y, z, oc))

    def to_dy(i):
        return i + (i // 2) * (5 - 2 * i)

    ld_basis.wait()
    gram()
    gram()

    ycps = {}

    def y_send(k):
        src = vblk(b0) if k == 2 else zoth
        cp = rcopy(src, vblk(b0), ys_s.at[k], ys_r.at[4 - k], dev(x, mod4(y + k), z, c))
        cp.start()
        sends.append(cp)
        ycps[4 - k] = cp

    def own_block(dy):
        x_right(dy).start()
        x_left(dy).start()
        d2d(0, dy).start()

    def ring(dy):
        x_right(dy).wait_recv()
        x_left(dy).wait_recv()
        x_far(dy).start()
        d2d(3, dy).start()
        d2d(1, dy).start()

    def mine(*which):
        mm1([blk(xx, dy, c) for xx, dy in which])

    def others(*which):
        for xo, dy in which:
            d2d(xo, dy).wait_recv()
        mm1([blk(mod4(x + xo), dy, oc) for xo, dy in which])

    for cp in zrecvs[0]:
        cp.wait_recv()
    y_send(1)
    y_send(3)
    for cp in zrecvs[1]:
        cp.wait_recv()
    own_block(0)
    y_send(2)
    ld_act.wait()
    mine((x, 0))
    ld_rest.wait()
    gram()
    ycps[1].wait_recv()
    own_block(1)
    ycps[3].wait_recv()
    own_block(3)
    ring(0)
    gram()
    mine((x, 1), (x, 3))
    ring(1)
    mine((xm, 0), (xp, 0))
    ycps[2].wait_recv()
    own_block(2)
    mine((xm, 1), (xp, 1))
    ring(3)
    gram()
    gram()
    others((0, 0), (0, 1), (0, 3))
    gram()
    others((3, 0), (1, 0))
    mine((x, 2), (xm, 3), (xp, 3))
    ring(2)
    mine((xm, 2), (xp, 2))
    x_far(0).wait_recv()
    d2d(2, 0).start()
    mine((xf, 0))
    gram()
    x_far(1).wait_recv()
    d2d(2, 1).start()
    mine((xf, 1))
    others((3, 1), (1, 1), (0, 2), (2, 0))
    x_far(3).wait_recv()
    d2d(2, 3).start()
    mine((xf, 3))
    others((3, 3), (1, 3), (3, 2), (1, 2), (2, 1))
    x_far(2).wait_recv()
    d2d(2, 2).start()
    mine((xf, 2))
    others((2, 3), (2, 2))
    gram_state = gram_state[0]

    lane8 = lax.broadcasted_iota(jnp.int32, (8, 128), 1)
    sub8 = lax.broadcasted_iota(jnp.int32, (8, 128), 0)
    zero4 = jnp.zeros((4, 128), F32)

    def lanes(v):
        return jnp.broadcast_to(jnp.sum(v, axis=1, keepdims=True), (8, 128))

    def pad(v):
        return jnp.concatenate([v, zero4], axis=0)

    def reduce_start(stage, buf, value, ss, rs):
        me, count = ((z * 2 + c, 8), (y, 4), (x, 4))[stage]
        buf[me] = value
        cps = []
        for k in range(1, count):
            t = lax.rem(me + k, count)
            d = (
                dev(x, y, t // 2, lax.rem(t, 2)) if stage == 0 else dev(x, t, z, c) if stage == 1 else dev(t, y, z, c)
            )
            cp = rcopy(buf.at[me], buf.at[me], ss.at[k], rs.at[k], d)
            cp.start()
            cps.append(cp)
        sends.extend(cps)
        return cps, buf, count

    def reduce_end(started):
        cps, buf, count = started
        for cp in cps:
            cp.wait_recv()
        parts = [buf[k] for k in range(count)]
        while len(parts) > 1:
            parts = [parts[k] + parts[k + 1] for k in range(0, len(parts), 2)]
        return parts[0]

    gup = jnp.zeros((8, 128), F32)
    gdn = jnp.zeros((8, 128), F32)
    for j in range(NB):
        gup = jnp.where(lane8 == j, lanes(gram_state[0][j]), gup)
        gdn = jnp.where(lane8 == j, lanes(pad(gram_state[1][j])), gdn)
    gram_sum = reduce_start(0, arz, jnp.concatenate([gup, gdn], axis=0), az_s, az_r)

    ld_curv.wait()

    for m in range(4):
        r = slice(m * 256, (m + 1) * 256)
        wt[:, r] = (curv[r, :] * acc[r, :]).T.astype(BF16)

    def mm2(b):
        return jnp.dot(wt[...], act[:, rows(b)], preferred_element_type=F32)

    def d2d2(i):
        return rcopy(dsend.at[i], drecv.at[i], d2_s.at[i], d2_r.at[i], dev(x, y, z, oc))

    def idx(xo, dy):
        return xo * 4 + dy

    def other(*which):
        ps = [mm2(blk(mod4(x + xo), dy, oc)).astype(BF16) for xo, dy in which]
        for (xo, dy), p in zip(which, ps):
            dsend[idx(xo, dy)] = p
        for xo, dy in which:
            d2d2(idx(xo, dy)).start()

    def chip_sums(*which):
        ps = [mm2(blk(mod4(x + xo), dy, c)) for xo, dy in which]
        for xo, dy in which:
            d2d2(idx(xo, dy)).wait_recv()
        return [p + drecv[idx(xo, dy)].astype(F32) for (xo, dy), p in zip(which, ps)]

    def far2(dy):
        odd = lax.rem(dy, 2)
        return rcopy(xfs.at[dy], xfr.at[dy], f2_s.at[dy], f2_r.at[dy], dev(mod4(x - 1 + 2 * odd), y, z, c))

    def right2(dy):
        return rcopy(xns.at[dy], xl.at[dy], n2_s.at[dy], l2_r.at[dy], dev(xp, y, z, c))

    def left2(dy):
        return rcopy(xns.at[4 + dy], xr.at[dy], n2_s.at[4 + dy], r2_r.at[dy], dev(xm, y, z, c))

    def far_send(*dys):
        for dy, s in zip(dys, chip_sums(*((2, dy) for dy in dys))):
            xfs[dy] = s.astype(BF16)
        for dy in dys:
            far2(dy).start()

    def near_send(*dys):
        for dy, s in zip(dys, chip_sums(*((1 + 2 * (dy % 2), dy) for dy in dys))):
            xns[(dy % 2) * 4 + dy] = s.astype(BF16)
        for dy in dys:
            (left2 if dy % 2 else right2)(dy).start()

    def near_add(*dys):
        sums = chip_sums(*((3 - 2 * (dy % 2), dy) for dy in dys))
        for dy in dys:
            far2(dy).wait_recv()
        for dy, s in zip(dys, sums):
            xns[(1 - dy % 2) * 4 + dy] = (s + xfr[dy].astype(F32)).astype(BF16)
        for dy in dys:
            (right2 if dy % 2 else left2)(dy).start()

    early, late = (2, 3), (1, 0)
    other((2, 2), (2, 3))
    other((2, 1), (2, 0))
    other((1, 2), (3, 3))
    far_send(*early)
    far_send(*late)
    other((3, 1), (1, 0))
    near_send(*early)
    other((3, 2), (1, 3))
    near_send(1)
    other((1, 1), (3, 0))
    gram_sum = reduce_start(1, ary, reduce_end(gram_sum), ay_s, ay_r)
    near_add(*early)
    other((0, 2), (0, 3))
    near_add(1)
    near_send(0)
    near_add(0)
    other((0, 1), (0, 0))
    gram_sum = reduce_start(2, arx, reduce_end(gram_sum), ax_s, ax_r)
    x_own = dict(zip((2, 3, 1, 0), chip_sums((0, 2), (0, 3), (0, 1), (0, 0))))

    def x_sum(dy):
        right2(dy).wait_recv()
        left2(dy).wait_recv()
        return x_own[dy] + xl[dy].astype(F32) + xr[dy].astype(F32)

    def y2(k):
        return rcopy(ysend.at[k], yrecv.at[4 - k], y2_s.at[k], y2_r.at[4 - k], dev(x, mod4(y + k), z, c))

    for k in (2, 3, 1):
        ysend[k] = x_sum(k).astype(BF16)
        cp = y2(k)
        cp.start()
        sends.append(cp)
    h_own = x_sum(0)
    y2(1).wait_recv()
    y2(3).wait_recv()
    h_oth = yrecv[1].astype(F32) + yrecv[3].astype(F32)
    zcps = []

    def z2(value, head, q):
        v = value.T.astype(BF16)
        for zz in range(4):
            zsend[zz, head] = v[zz * 64 : (zz + 1) * 64, :]
        for k in (2, 1, 3):
            zt = mod4(z + k)
            n = q * 3 + k - 1
            cp = rcopy(zsend.at[zt, head], zrecv.at[z, head], z2_s.at[n], z2_r.at[n], dev(x, y, zt, c))
            cp.start()
            sends.append(cp)
            zcps.append(cp)

    z2(h_oth, 1 - yl, 0)
    y2(2).wait_recv()
    z2(h_own + yrecv[2].astype(F32), yl, 1)
    zrecv[z] = zsend[z]
    for cp in zcps:
        cp.wait_recv()

    for zz in range(4):
        for hl in range(2):
            for kv in range(2):
                v = zrecv[zz, hl, :, kv * 128 : (kv + 1) * 128].astype(F32) * (1.0 / TOKENS)
                curved[pl.ds(2 * (hl * 4 + zz) + kv, 64, stride=16), :] = v

    def dot_chunk(i, carry):
        tops, bots, sq = carry
        tops, bots = list(tops), list(bots)
        for u in range(4):
            t = curved[pl.ds(pl.multiple_of(i * 32 + u * 8, 8), 8), :]
            sq = sq + t * t
            for s in range(8):
                cols = pl.ds(pl.multiple_of(i * 4096 + u * 1024 + s * 128, 128), 128)
                row = t[s : s + 1]
                tops[s % 4] = tops[s % 4] + basis[0:8, cols] * jnp.broadcast_to(row, (8, 128))
                bots[s % 4] = bots[s % 4] + basis[8:12, cols] * jnp.broadcast_to(row, (4, 128))
        return tuple(tops), tuple(bots), sq

    tops, bots, sq = lax.fori_loop(
        0,
        32,
        dot_chunk,
        (
            tuple(jnp.zeros((8, 128), F32) for _ in range(4)),
            tuple(jnp.zeros((4, 128), F32) for _ in range(4)),
            jnp.zeros((8, 128), F32),
        ),
    )
    top = (tops[0] + tops[1]) + (tops[2] + tops[3])
    bot = (bots[0] + bots[1]) + (bots[2] + bots[3])

    row = jnp.sum(
        jnp.where(lane8 == sub8, lanes(top), 0.0)
        + jnp.where(lane8 == sub8 + 8, lanes(pad(bot)), 0.0)
        + jnp.where(lane8 == NB, lanes(sq), 0.0),
        axis=0,
        keepdims=True,
    )
    row = reduce_end(reduce_start(0, crz, row, cz_s, cz_r))
    row = reduce_end(reduce_start(1, cry, row, cy_s, cy_r))
    row = reduce_end(reduce_start(2, crx, row, cx_s, cx_r))
    row = row * (1.0 / PARAMS)
    tot = reduce_end(gram_sum) * (1.0 / PARAMS)
    gt, gb = tot[0:8], tot[8:16]
    lane1 = lax.broadcasted_iota(jnp.int32, (1, 128), 1)
    crow = jnp.where(lane1 < NB, row, 0.0)
    ct = lanes(jnp.where(lane8 == sub8, jnp.broadcast_to(crow, (8, 128)), 0.0))
    cb = lanes(jnp.where(lane8 == sub8 + 8, jnp.broadcast_to(crow, (8, 128)), 0.0))
    gc = jnp.sum(gt * ct + gb * cb, axis=0, keepdims=True)
    cgc = jnp.sum(crow * gc, axis=1, keepdims=True)
    cc = jnp.sum(crow * crow, axis=1, keepdims=True)
    squares = jnp.sum(jnp.where(lane1 == NB, row, 0.0), axis=1, keepdims=True)
    norm = jnp.sqrt(squares - 2.0 * cc + cgc + 1e-06)
    inv = jnp.broadcast_to(1.0 / norm, (8, 128))
    hess_ref[...] = jnp.where(lane1 == NB, jnp.broadcast_to(norm, (1, 128)), crow)

    def res_chunk(i, _):
        for u in range(4):
            t = []
            for s in range(8):
                cols = pl.ds(pl.multiple_of(i * 4096 + u * 1024 + s * 128, 128), 128)
                t.append(basis[0:8, cols] * ct + pad(basis[8:12, cols]) * cb)
            for sh in (4, 2, 1):
                keep = lax.rem(sub8 // sh, 2) == 0
                t = [
                    jnp.where(
                        keep,
                        t[s] + pltpu.roll(t[s], 8 - sh, 0),
                        t[s + sh] + pltpu.roll(t[s + sh], sh, 0),
                    )
                    for s in range(sh)
                ]
            r = pl.ds(pl.multiple_of(i * 32 + u * 8, 8), 8)
            out_ref[r, :] = (curved[r, :] - t[0]) * inv
        return 0

    lax.fori_loop(0, 32, res_chunk, 0)

    for cp in sends:
        cp.wait_send()

    def drain(dy, _):
        x_right(dy).wait_send()
        x_left(dy).wait_send()
        x_far(dy).wait_send()
        far2(dy).wait_send()
        right2(dy).wait_send()
        left2(dy).wait_send()
        for xo in range(4):
            d2d(xo, dy).wait_send()
            d2d2(xo * 4 + dy).wait_send()
        return 0

    lax.fori_loop(0, 4, drain, 0)


def body(activations, curvature, basis, krylov):
    dma = pltpu.SemaphoreType.DMA
    vm = pltpu.VMEM
    anyspace = pl.BlockSpec(memory_space=pltpu.HBM)
    vspace = pl.BlockSpec(memory_space=pltpu.VMEM)
    blocks = lambda n: vm((n, 256, 256), BF16)
    out, hess = pl.pallas_call(
        kernel,
        out_shape=(jax.ShapeDtypeStruct((1024, 128), F32), jax.ShapeDtypeStruct((1, 128), F32)),
        in_specs=[anyspace] * 4,
        out_specs=(vspace, vspace),
        scratch_shapes=[
            vm((1024, 8192), BF16),
            vm((1024, 256), F32),
            vm((NB, 131072), F32),
            vm((1024, 128), F32),
            vm((8192, 256), BF16),
            vm((4, 2, 64, 256), BF16),
            vm((256, 256), BF16),
            vm((1024, 256), F32),
            vm((256, 1024), BF16),
            blocks(16),
            blocks(16),
            blocks(4),
            blocks(8),
            blocks(4),
            blocks(4),
            blocks(4),
            blocks(4),
            blocks(4),
            vm((4, 2, 64, 256), BF16),
            vm((4, 2, 64, 256), BF16),
            vm((1024, 128), F32),
            vm((8, 16, 128), F32),
            vm((4, 16, 128), F32),
            vm((4, 16, 128), F32),
            vm((8, 1, 128), F32),
            vm((4, 1, 128), F32),
            vm((4, 1, 128), F32),
            dma((5,)),
            dma((6,)),
            dma((6,)),
            dma((4,)),
            dma((4,)),
            dma((4,)),
            dma((4,)),
            dma((4,)),
            dma((4,)),
            dma((4,)),
            dma((4,)),
            dma((16,)),
            dma((16,)),
            dma((16,)),
            dma((16,)),
            dma((4,)),
            dma((4,)),
            dma((8,)),
            dma((4,)),
            dma((4,)),
            dma((4,)),
            dma((4,)),
            dma((6,)),
            dma((6,)),
            dma((8,)),
            dma((8,)),
            dma((4,)),
            dma((4,)),
            dma((4,)),
            dma((4,)),
            dma((8,)),
            dma((8,)),
            dma((4,)),
            dma((4,)),
            dma((4,)),
            dma((4,)),
        ],
        compiler_params=pltpu.CompilerParams(
            collective_id=0, has_side_effects=True, vmem_limit_bytes=VMEM_BYTES
        ),
    )(activations, curvature, basis, krylov.reshape(1024, 128))
    return out.reshape(131072), hess[0, :13]


def solution(mesh):
    placed = (P("dp", None), P("dp", "mp"), P(None, ("dp", "mp")), P(("dp", "mp")))
    return jax.shard_map(
        body, mesh=mesh, in_specs=placed, out_specs=(P(("dp", "mp")), P()), check_vma=False
    )
```

```python
import functools

import jax
import jax.numpy as jnp
from jax import lax
from jax.experimental import pallas as pl
from jax.experimental.pallas import tpu as pltpu
from jax.sharding import PartitionSpec as P

MESH = pl.DeviceIdType.MESH
TOKENS = 16384
PARAMS = 16777216
NB = 12
F32 = jnp.float32
BF16 = jnp.bfloat16
GRAM_UNROLL = 4
VMEM_BYTES = 55_750_000
GRAM_PIECES = 8
BLK = 256


def kernel(
    act_hbm, curv_hbm, basis_hbm, kry_hbm, out_ref, hess_ref,
    act, curv, basis, kry_ref, vmat, ksend, zoth, acc, wt,
    dsend, drecv, xfs, xns, xfr, xl, xr, ysend, yrecv, zsend, zrecv, curved,
    yfs, yfr, arz, ary, arx, crz, cry, crx,
    lsem, zs_s, zs_r, ys_s, ys_r, xr_s, xr_r, xl_s, xl_r, xf_s, xf_r, d_s, d_r,
    d2_s, d2_r, f2_s, f2_r, n2_s, l2_r, r2_r, y2_s, y2_r, z2_s, z2_r,
    az_s, az_r, ay_s, ay_r, ax_s, ax_r, cz_s, cz_r, cy_s, cy_r, cx_s, cx_r, yf_s, yf_r,
):
    dp = lax.axis_index("dp")
    mp = lax.axis_index("mp")
    c = lax.rem(dp, 2)
    x = lax.rem(dp // 2, 4)
    y = (dp // 8) * 2 + mp // 4
    yl = mp // 4
    z = lax.rem(mp, 4)
    oc = 1 - c

    def dev(xx, yy, zz, cc):
        return {"dp": ((yy // 2) * 4 + xx) * 2 + cc, "mp": lax.rem(yy, 2) * 4 + zz}

    def mod4(v):
        return lax.rem(v + 8, 4)

    def blk(xx, dy, cc):
        yy = mod4(y + dy)
        return (((yy // 2) * 4 + xx) * 2 + cc) * 2 + lax.rem(yy, 2)

    def rows(b):
        return pl.ds(pl.multiple_of(b * BLK, BLK), BLK)

    def rcopy(src, dst, ss, rs, device):
        return pltpu.make_async_remote_copy(
            src_ref=src, dst_ref=dst, send_sem=ss, recv_sem=rs, device_id=device, device_id_type=MESH
        )

    first, rest = pl.ds(0, 32768), pl.ds(32768, 98304)
    ld_basis = pltpu.make_async_copy(basis_hbm.at[:, first], basis.at[:, first], lsem.at[0])
    ld_rest = pltpu.make_async_copy(basis_hbm.at[:, rest], basis.at[:, rest], lsem.at[4])
    ld_act = pltpu.make_async_copy(act_hbm, act, lsem.at[1])
    ld_curv = pltpu.make_async_copy(curv_hbm, curv, lsem.at[2])
    ld_kry = pltpu.make_async_copy(kry_hbm, kry_ref, lsem.at[3])
    ld_kry.start()
    ld_basis.start()
    ld_act.start()
    ld_rest.start()
    ld_curv.start()

    barrier = pltpu.get_barrier_semaphore()
    partners = [dev(x, y, z, oc)]
    for k in (1, 2, 3):
        partners.append(dev(x, y, mod4(z + k), c))
        partners.append(dev(x, y, mod4(z + k), oc))
        partners.append(dev(x, mod4(y + k), z, c))
        partners.append(dev(mod4(x + k), y, z, c))
    for p in partners:
        pl.semaphore_signal(barrier, inc=1, device_id=p, device_id_type=MESH)

    acc[...] = jnp.zeros_like(acc)
    ld_kry.wait()

    for h in range(8):
        for kv in range(2):
            v = kry_ref[pl.ds(2 * h + kv, 64, stride=16), :]
            ksend[h % 4, h // 4, :, kv * 128 : (kv + 1) * 128] = v.astype(BF16)
    b0 = blk(x, 0, c)
    zrow = pl.multiple_of(z * 64, 64)
    vrow = pl.multiple_of(b0 * BLK + z * 64, 64)
    vmat[pl.ds(vrow, 64), :] = ksend[z, yl]
    zoth[pl.ds(zrow, 64), :] = ksend[z, 1 - yl]

    pl.semaphore_wait(barrier, len(partners))

    sends = []
    zrecvs = ([], [])
    for q in range(2):
        for k in (2, 1, 3):
            zt = mod4(z + k)
            if q == 0:
                src, dst = ksend.at[zt, 1 - yl], zoth.at[pl.ds(zrow, 64), :]
            else:
                src, dst = ksend.at[zt, yl], vmat.at[pl.ds(vrow, 64), :]
            n = q * 3 + k - 1
            cp = rcopy(src, dst, zs_s.at[n], zs_r.at[n], dev(x, y, zt, c))
            cp.start()
            sends.append(cp)
            zrecvs[q].append(cp)

    def gram_chunk(i, carry):
        top, bot = carry
        top, bot = list(top), list(bot)
        for u in range(GRAM_UNROLL):
            cols = pl.ds(pl.multiple_of(i * (128 * GRAM_UNROLL) + u * 128, 128), 128)
            a = basis[0:8, cols]
            b = basis[8:12, cols]
            for j in range(NB):
                row = a[j : j + 1] if j < 8 else b[j - 8 : j - 7]
                top[j] = top[j] + a * jnp.broadcast_to(row, (8, 128))
                bot[j] = bot[j] + b * jnp.broadcast_to(row, (4, 128))
        return tuple(top), tuple(bot)

    gram_state = [
        (
            tuple(jnp.zeros((8, 128), F32) for _ in range(NB)),
            tuple(jnp.zeros((4, 128), F32) for _ in range(NB)),
        )
    ]
    steps = 1024 // GRAM_UNROLL // GRAM_PIECES
    done = [0]

    def gram():
        n = done[0]
        gram_state[0] = lax.fori_loop(n * steps, (n + 1) * steps, gram_chunk, gram_state[0])
        done[0] = n + 1

    def vblk(b):
        return vmat.at[rows(b), :]

    def mm1(bs):
        for m in range(2):
            r = slice(m * 512, (m + 1) * 512)
            p = [jnp.dot(act[r, rows(b)], vmat[rows(b), :], preferred_element_type=F32) for b in bs]
            acc[r, :] += functools.reduce(jnp.add, p)

    xp, xm, xf = mod4(x + 1), mod4(x - 1), mod4(x + 2)

    def x_right(dy):
        b = blk(x, dy, c)
        return rcopy(vblk(b), vblk(b), xr_s.at[dy], xr_r.at[dy], dev(xp, y, z, c))

    yf = dev(x, mod4(y + 2), z, c)

    def x_left(dy):
        b = blk(x, dy, c)
        return rcopy(vblk(b), vblk(b), xl_s.at[dy], xl_r.at[dy], dev(xm, y, z, c))

    def x_far(dy):
        odd = lax.rem(dy, 2)
        b = blk(mod4(x - 1 + 2 * odd), dy, c)
        return rcopy(vblk(b), vblk(b), xf_s.at[dy], xf_r.at[dy], dev(mod4(x + 1 - 2 * odd), y, z, c))

    def d2d(xo, dy):
        b = blk(mod4(x + xo), dy, c)
        return rcopy(vblk(b), vblk(b), d_s.at[xo * 4 + dy], d_r.at[xo * 4 + dy], dev(x, y, z, oc))

    def to_dy(i):
        return i + (i // 2) * (5 - 2 * i)

    ld_basis.wait()
    gram()
    gram()

    ycps = {}

    def y_send(k):
        src = vblk(b0) if k == 2 else zoth
        cp = rcopy(src, vblk(b0), ys_s.at[k], ys_r.at[4 - k], dev(x, mod4(y + k), z, c))
        cp.start()
        sends.append(cp)
        ycps[4 - k] = cp

    def own_block(dy):
        x_right(dy).start()
        x_left(dy).start()
        d2d(0, dy).start()

    def ring(dy):
        x_right(dy).wait_recv()
        x_left(dy).wait_recv()
        x_far(dy).start()
        d2d(3, dy).start()
        d2d(1, dy).start()

    def mine(*which):
        mm1([blk(xx, dy, c) for xx, dy in which])

    def others(*which):
        for xo, dy in which:
            d2d(xo, dy).wait_recv()
        mm1([blk(mod4(x + xo), dy, oc) for xo, dy in which])

    for cp in zrecvs[0]:
        cp.wait_recv()
    y_send(1)
    y_send(3)
    for cp in zrecvs[1]:
        cp.wait_recv()
    own_block(0)
    y_send(2)
    ld_act.wait()
    mine((x, 0))
    ld_rest.wait()
    gram()
    ycps[1].wait_recv()
    own_block(1)
    ycps[3].wait_recv()
    own_block(3)
    ring(0)
    gram()
    mine((x, 1), (x, 3))
    ring(1)
    mine((xm, 0), (xp, 0))
    ycps[2].wait_recv()
    own_block(2)
    mine((xm, 1), (xp, 1))
    ring(3)
    gram()
    gram()
    others((0, 0), (0, 1), (0, 3))
    gram()
    others((3, 0), (1, 0))
    mine((x, 2), (xm, 3), (xp, 3))
    ring(2)
    mine((xm, 2), (xp, 2))
    x_far(0).wait_recv()
    d2d(2, 0).start()
    mine((xf, 0))
    gram()
    x_far(1).wait_recv()
    d2d(2, 1).start()
    mine((xf, 1))
    others((3, 1), (1, 1), (0, 2), (2, 0))
    x_far(3).wait_recv()
    d2d(2, 3).start()
    mine((xf, 3))
    others((3, 3), (1, 3), (3, 2), (1, 2), (2, 1))
    x_far(2).wait_recv()
    d2d(2, 2).start()
    mine((xf, 2))
    others((2, 3), (2, 2))
    gram_state = gram_state[0]

    lane8 = lax.broadcasted_iota(jnp.int32, (8, 128), 1)
    sub8 = lax.broadcasted_iota(jnp.int32, (8, 128), 0)
    zero4 = jnp.zeros((4, 128), F32)

    def lanes(v):
        return jnp.broadcast_to(jnp.sum(v, axis=1, keepdims=True), (8, 128))

    def pad(v):
        return jnp.concatenate([v, zero4], axis=0)

    def reduce_start(stage, buf, value, ss, rs):
        me, count = ((z * 2 + c, 8), (y, 4), (x, 4))[stage]
        buf[me] = value
        cps = []
        for k in range(1, count):
            t = lax.rem(me + k, count)
            d = (
                dev(x, y, t // 2, lax.rem(t, 2)) if stage == 0 else dev(x, t, z, c) if stage == 1 else dev(t, y, z, c)
            )
            cp = rcopy(buf.at[me], buf.at[me], ss.at[k], rs.at[k], d)
            cp.start()
            cps.append(cp)
        sends.extend(cps)
        return cps, buf, count

    def reduce_end(started):
        cps, buf, count = started
        for cp in cps:
            cp.wait_recv()
        parts = [buf[k] for k in range(count)]
        while len(parts) > 1:
            parts = [parts[k] + parts[k + 1] for k in range(0, len(parts), 2)]
        return parts[0]

    gup = jnp.zeros((8, 128), F32)
    gdn = jnp.zeros((8, 128), F32)
    for j in range(NB):
        gup = jnp.where(lane8 == j, lanes(gram_state[0][j]), gup)
        gdn = jnp.where(lane8 == j, lanes(pad(gram_state[1][j])), gdn)
    gram_sum = reduce_start(0, arz, jnp.concatenate([gup, gdn], axis=0), az_s, az_r)

    ld_curv.wait()

    for m in range(4):
        r = slice(m * 256, (m + 1) * 256)
        wt[:, r] = (curv[r, :] * acc[r, :]).T.astype(BF16)

    def mm2(b):
        return jnp.dot(wt[...], act[:, rows(b)], preferred_element_type=F32)

    def d2d2(i):
        return rcopy(dsend.at[i], drecv.at[i], d2_s.at[i], d2_r.at[i], dev(x, y, z, oc))

    def idx(xo, dy):
        return xo * 4 + dy

    def other(*which):
        ps = [mm2(blk(mod4(x + xo), dy, oc)).astype(BF16) for xo, dy in which]
        for (xo, dy), p in zip(which, ps):
            dsend[idx(xo, dy)] = p
        for xo, dy in which:
            d2d2(idx(xo, dy)).start()

    def chip_sums(*which):
        ps = [mm2(blk(mod4(x + xo), dy, c)) for xo, dy in which]
        for xo, dy in which:
            d2d2(idx(xo, dy)).wait_recv()
        return [p + drecv[idx(xo, dy)].astype(F32) for (xo, dy), p in zip(which, ps)]

    def far2(dy):
        odd = lax.rem(dy, 2)
        return rcopy(xfs.at[dy], xfr.at[dy], f2_s.at[dy], f2_r.at[dy], dev(mod4(x - 1 + 2 * odd), y, z, c))

    def right2(dy):
        return rcopy(xns.at[dy], xl.at[dy], n2_s.at[dy], l2_r.at[dy], dev(xp, y, z, c))

    def left2(dy):
        return rcopy(xns.at[4 + dy], xr.at[dy], n2_s.at[4 + dy], r2_r.at[dy], dev(xm, y, z, c))

    def far_send(*dys):
        for dy, s in zip(dys, chip_sums(*((2, dy) for dy in dys))):
            if dy == 0:
                y_far(0).wait_recv()
                s = s + yfr[0].astype(F32)
            xfs[dy] = s.astype(BF16)
        for dy in dys:
            far2(dy).start()

    def near_send(*dys):
        for dy, s in zip(dys, chip_sums(*((1 + 2 * (dy % 2), dy) for dy in dys))):
            if dy == 0:
                y_far(1).wait_recv()
                s = s + yfr[1].astype(F32)
            xns[(dy % 2) * 4 + dy] = s.astype(BF16)
        for dy in dys:
            (left2 if dy % 2 else right2)(dy).start()

    def near_add(*dys):
        sums = chip_sums(*((3 - 2 * (dy % 2), dy) for dy in dys))
        for dy, s in zip(dys, sums):
            if dy != 2:
                far2(dy).wait_recv()
                s = s + xfr[dy].astype(F32)
            xns[(1 - dy % 2) * 4 + dy] = s.astype(BF16)
        for dy in dys:
            (right2 if dy % 2 else left2)(dy).start()

    def y_far(n):
        return rcopy(yfs.at[n], yfr.at[n], yf_s.at[n], yf_r.at[n], yf)

    other((2, 2), (1, 2))
    other((2, 3), (2, 1))
    other((3, 3), (3, 1))
    for n, s in enumerate(chip_sums((2, 2), (1, 2))):
        yfs[n] = s.astype(BF16)
        y_far(n).start()
    far_send(3, 1)
    near_send(3, 1)
    other((2, 0), (1, 3))
    other((3, 2), (1, 1))
    far_send(0)
    near_add(3)
    near_add(2)
    other((1, 0), (3, 0))
    near_add(1)
    other((0, 2), (0, 3))
    gram_sum = reduce_start(1, ary, reduce_end(gram_sum), ay_s, ay_r)
    near_send(0)
    other((0, 1), (0, 0))
    gram_sum = reduce_start(2, arx, reduce_end(gram_sum), ax_s, ax_r)
    x_own = dict(zip((2, 3, 1, 0), chip_sums((0, 2), (0, 3), (0, 1), (0, 0))))
    near_add(0)

    def x_sum(dy):
        left2(dy).wait_recv()
        s = x_own[dy] + xr[dy].astype(F32)
        if dy != 2:
            right2(dy).wait_recv()
            s = s + xl[dy].astype(F32)
        return s

    def y2(k):
        return rcopy(ysend.at[k], yrecv.at[4 - k], y2_s.at[k], y2_r.at[4 - k], dev(x, mod4(y + k), z, c))

    for k in (2, 3, 1):
        ysend[k] = x_sum(k).astype(BF16)
        cp = y2(k)
        cp.start()
        sends.append(cp)
    h_own = x_sum(0)
    y2(1).wait_recv()
    y2(3).wait_recv()
    h_oth = yrecv[1].astype(F32) + yrecv[3].astype(F32)
    zcps = []

    def z2(value, head, q):
        v = value.T.astype(BF16)
        for zz in range(4):
            zsend[zz, head] = v[zz * 64 : (zz + 1) * 64, :]
        for k in (2, 1, 3):
            zt = mod4(z + k)
            n = q * 3 + k - 1
            cp = rcopy(zsend.at[zt, head], zrecv.at[z, head], z2_s.at[n], z2_r.at[n], dev(x, y, zt, c))
            cp.start()
            sends.append(cp)
            zcps.append(cp)

    z2(h_oth, 1 - yl, 0)
    y2(2).wait_recv()
    z2(h_own + yrecv[2].astype(F32), yl, 1)
    zrecv[z] = zsend[z]
    for cp in zcps:
        cp.wait_recv()

    for zz in range(4):
        for hl in range(2):
            for kv in range(2):
                v = zrecv[zz, hl, :, kv * 128 : (kv + 1) * 128].astype(F32) * (1.0 / TOKENS)
                curved[pl.ds(2 * (hl * 4 + zz) + kv, 64, stride=16), :] = v

    def dot_chunk(i, carry):
        tops, bots, sq = carry
        tops, bots = list(tops), list(bots)
        for u in range(4):
            t = curved[pl.ds(pl.multiple_of(i * 32 + u * 8, 8), 8), :]
            sq = sq + t * t
            for s in range(8):
                cols = pl.ds(pl.multiple_of(i * 4096 + u * 1024 + s * 128, 128), 128)
                row = t[s : s + 1]
                tops[s % 4] = tops[s % 4] + basis[0:8, cols] * jnp.broadcast_to(row, (8, 128))
                bots[s % 4] = bots[s % 4] + basis[8:12, cols] * jnp.broadcast_to(row, (4, 128))
        return tuple(tops), tuple(bots), sq

    tops, bots, sq = lax.fori_loop(
        0,
        32,
        dot_chunk,
        (
            tuple(jnp.zeros((8, 128), F32) for _ in range(4)),
            tuple(jnp.zeros((4, 128), F32) for _ in range(4)),
            jnp.zeros((8, 128), F32),
        ),
    )
    top = (tops[0] + tops[1]) + (tops[2] + tops[3])
    bot = (bots[0] + bots[1]) + (bots[2] + bots[3])

    row = jnp.sum(
        jnp.where(lane8 == sub8, lanes(top), 0.0)
        + jnp.where(lane8 == sub8 + 8, lanes(pad(bot)), 0.0)
        + jnp.where(lane8 == NB, lanes(sq), 0.0),
        axis=0,
        keepdims=True,
    )
    row = reduce_end(reduce_start(0, crz, row, cz_s, cz_r))
    row = reduce_end(reduce_start(1, cry, row, cy_s, cy_r))
    row = reduce_end(reduce_start(2, crx, row, cx_s, cx_r))
    row = row * (1.0 / PARAMS)
    tot = reduce_end(gram_sum) * (1.0 / PARAMS)
    gt, gb = tot[0:8], tot[8:16]
    lane1 = lax.broadcasted_iota(jnp.int32, (1, 128), 1)
    crow = jnp.where(lane1 < NB, row, 0.0)
    ct = lanes(jnp.where(lane8 == sub8, jnp.broadcast_to(crow, (8, 128)), 0.0))
    cb = lanes(jnp.where(lane8 == sub8 + 8, jnp.broadcast_to(crow, (8, 128)), 0.0))
    gc = jnp.sum(gt * ct + gb * cb, axis=0, keepdims=True)
    cgc = jnp.sum(crow * gc, axis=1, keepdims=True)
    cc = jnp.sum(crow * crow, axis=1, keepdims=True)
    squares = jnp.sum(jnp.where(lane1 == NB, row, 0.0), axis=1, keepdims=True)
    norm = jnp.sqrt(squares - 2.0 * cc + cgc + 1e-06)
    inv = jnp.broadcast_to(1.0 / norm, (8, 128))
    hess_ref[...] = jnp.where(lane1 == NB, jnp.broadcast_to(norm, (1, 128)), crow)

    def res_chunk(i, _):
        for u in range(4):
            t = []
            for s in range(8):
                cols = pl.ds(pl.multiple_of(i * 4096 + u * 1024 + s * 128, 128), 128)
                t.append(basis[0:8, cols] * ct + pad(basis[8:12, cols]) * cb)
            for sh in (4, 2, 1):
                keep = lax.rem(sub8 // sh, 2) == 0
                t = [
                    jnp.where(
                        keep,
                        t[s] + pltpu.roll(t[s], 8 - sh, 0),
                        t[s + sh] + pltpu.roll(t[s + sh], sh, 0),
                    )
                    for s in range(sh)
                ]
            r = pl.ds(pl.multiple_of(i * 32 + u * 8, 8), 8)
            out_ref[r, :] = (curved[r, :] - t[0]) * inv
        return 0

    lax.fori_loop(0, 32, res_chunk, 0)

    for cp in sends:
        cp.wait_send()

    for dy in range(4):
        x_right(dy).wait_send()
        x_left(dy).wait_send()
        x_far(dy).wait_send()
        left2(dy).wait_send()
        if dy != 2:
            far2(dy).wait_send()
            right2(dy).wait_send()
        for xo in range(4):
            d2d(xo, dy).wait_send()
            d2d2(xo * 4 + dy).wait_send()
    for n in range(2):
        y_far(n).wait_send()


def body(activations, curvature, basis, krylov):
    dma = pltpu.SemaphoreType.DMA
    vm = pltpu.VMEM
    anyspace = pl.BlockSpec(memory_space=pltpu.HBM)
    vspace = pl.BlockSpec(memory_space=pltpu.VMEM)
    blocks = lambda n: vm((n, 256, 256), BF16)
    out, hess = pl.pallas_call(
        kernel,
        out_shape=(jax.ShapeDtypeStruct((1024, 128), F32), jax.ShapeDtypeStruct((1, 128), F32)),
        in_specs=[anyspace] * 4,
        out_specs=(vspace, vspace),
        scratch_shapes=[
            vm((1024, 8192), BF16),
            vm((1024, 256), F32),
            vm((NB, 131072), F32),
            vm((1024, 128), F32),
            vm((8192, 256), BF16),
            vm((4, 2, 64, 256), BF16),
            vm((256, 256), BF16),
            vm((1024, 256), F32),
            vm((256, 1024), BF16),
            blocks(16),
            blocks(16),
            blocks(4),
            blocks(8),
            blocks(4),
            blocks(4),
            blocks(4),
            blocks(4),
            blocks(4),
            vm((4, 2, 64, 256), BF16),
            vm((4, 2, 64, 256), BF16),
            vm((1024, 128), F32),
            blocks(2),
            blocks(2),
            vm((8, 16, 128), F32),
            vm((4, 16, 128), F32),
            vm((4, 16, 128), F32),
            vm((8, 1, 128), F32),
            vm((4, 1, 128), F32),
            vm((4, 1, 128), F32),
            dma((5,)),
            dma((6,)),
            dma((6,)),
            dma((4,)),
            dma((4,)),
            dma((4,)),
            dma((4,)),
            dma((4,)),
            dma((4,)),
            dma((4,)),
            dma((4,)),
            dma((16,)),
            dma((16,)),
            dma((16,)),
            dma((16,)),
            dma((4,)),
            dma((4,)),
            dma((8,)),
            dma((4,)),
            dma((4,)),
            dma((4,)),
            dma((4,)),
            dma((6,)),
            dma((6,)),
            dma((8,)),
            dma((8,)),
            dma((4,)),
            dma((4,)),
            dma((4,)),
            dma((4,)),
            dma((8,)),
            dma((8,)),
            dma((4,)),
            dma((4,)),
            dma((4,)),
            dma((4,)),
            dma((2,)),
            dma((2,)),
        ],
        compiler_params=pltpu.CompilerParams(
            collective_id=0, has_side_effects=True, vmem_limit_bytes=VMEM_BYTES
        ),
    )(activations, curvature, basis, krylov.reshape(1024, 128))
    return out.reshape(131072), hess[0, :13]


def solution(mesh):
    placed = (P("dp", None), P("dp", "mp"), P(None, ("dp", "mp")), P(("dp", "mp")))
    return jax.shard_map(
        body, mesh=mesh, in_specs=placed, out_specs=(P(("dp", "mp")), P()), check_vma=False
    )
```

```python
import functools

import jax
import jax.numpy as jnp
from jax import lax
from jax.experimental import pallas as pl
from jax.experimental.pallas import tpu as pltpu
from jax.sharding import PartitionSpec as P

MESH = pl.DeviceIdType.MESH
TOKENS = 16384
PARAMS = 16777216
NB = 12
F32 = jnp.float32
BF16 = jnp.bfloat16
GRAM_UNROLL = 4
VMEM_BYTES = 55_750_000
GRAM_PIECES = 8
BLK = 256


def kernel(
    act_hbm, curv_hbm, basis_hbm, kry_hbm, out_ref, hess_ref,
    act, curv, basis, kry_ref, vmat, ksend, zoth, acc, wt,
    dsend, drecv, xfs, xns, xfr, xl, xr, ysend, yrecv, zsend, zrecv, curved,
    yfs, yfr, arz, ary, arx, crz, cry, crx,
    lsem, zs_s, zs_r, ys_s, ys_r, xr_s, xr_r, xl_s, xl_r, xf_s, xf_r, d_s, d_r,
    d2_s, d2_r, f2_s, f2_r, n2_s, l2_r, r2_r, y2_s, y2_r, z2_s, z2_r,
    az_s, az_r, ay_s, ay_r, ax_s, ax_r, cz_s, cz_r, cy_s, cy_r, cx_s, cx_r, yf_s, yf_r,
):
    dp = lax.axis_index("dp")
    mp = lax.axis_index("mp")
    c = lax.rem(dp, 2)
    x = lax.rem(dp // 2, 4)
    y = (dp // 8) * 2 + mp // 4
    yl = mp // 4
    z = lax.rem(mp, 4)
    oc = 1 - c

    def dev(xx, yy, zz, cc):
        return {"dp": ((yy // 2) * 4 + xx) * 2 + cc, "mp": lax.rem(yy, 2) * 4 + zz}

    def mod4(v):
        return lax.rem(v + 8, 4)

    def blk(xx, dy, cc):
        yy = mod4(y + dy)
        return (((yy // 2) * 4 + xx) * 2 + cc) * 2 + lax.rem(yy, 2)

    def rows(b):
        return pl.ds(pl.multiple_of(b * BLK, BLK), BLK)

    def rcopy(src, dst, ss, rs, device):
        return pltpu.make_async_remote_copy(
            src_ref=src, dst_ref=dst, send_sem=ss, recv_sem=rs, device_id=device, device_id_type=MESH
        )

    first, rest = pl.ds(0, 32768), pl.ds(32768, 98304)
    ld_basis = pltpu.make_async_copy(basis_hbm.at[:, first], basis.at[:, first], lsem.at[0])
    ld_rest = pltpu.make_async_copy(basis_hbm.at[:, rest], basis.at[:, rest], lsem.at[4])
    ld_act = pltpu.make_async_copy(act_hbm, act, lsem.at[1])
    ld_curv = pltpu.make_async_copy(curv_hbm, curv, lsem.at[2])
    ld_kry = pltpu.make_async_copy(kry_hbm, kry_ref, lsem.at[3])
    ld_kry.start()
    ld_basis.start()
    ld_act.start()
    ld_rest.start()
    ld_curv.start()

    barrier = pltpu.get_barrier_semaphore()
    partners = [dev(x, y, z, oc)]
    for k in (1, 2, 3):
        partners.append(dev(x, y, mod4(z + k), c))
        partners.append(dev(x, y, mod4(z + k), oc))
        partners.append(dev(x, mod4(y + k), z, c))
        partners.append(dev(mod4(x + k), y, z, c))
    for p in partners:
        pl.semaphore_signal(barrier, inc=1, device_id=p, device_id_type=MESH)

    acc[...] = jnp.zeros_like(acc)
    ld_kry.wait()

    for h in range(8):
        for kv in range(2):
            v = kry_ref[pl.ds(2 * h + kv, 64, stride=16), :]
            ksend[h % 4, h // 4, :, kv * 128 : (kv + 1) * 128] = v.astype(BF16)
    b0 = blk(x, 0, c)
    zrow = pl.multiple_of(z * 64, 64)
    vrow = pl.multiple_of(b0 * BLK + z * 64, 64)
    vmat[pl.ds(vrow, 64), :] = ksend[z, yl]
    zoth[pl.ds(zrow, 64), :] = ksend[z, 1 - yl]

    pl.semaphore_wait(barrier, len(partners))

    sends = []
    zrecvs = ([], [])
    for q in range(2):
        for k in (2, 1, 3):
            zt = mod4(z + k)
            if q == 0:
                src, dst = ksend.at[zt, 1 - yl], zoth.at[pl.ds(zrow, 64), :]
            else:
                src, dst = ksend.at[zt, yl], vmat.at[pl.ds(vrow, 64), :]
            n = q * 3 + k - 1
            cp = rcopy(src, dst, zs_s.at[n], zs_r.at[n], dev(x, y, zt, c))
            cp.start()
            sends.append(cp)
            zrecvs[q].append(cp)

    def gram_chunk(i, carry):
        top, bot = carry
        top, bot = list(top), list(bot)
        for u in range(GRAM_UNROLL):
            cols = pl.ds(pl.multiple_of(i * (128 * GRAM_UNROLL) + u * 128, 128), 128)
            a = basis[0:8, cols]
            b = basis[8:12, cols]
            for j in range(NB):
                row = a[j : j + 1] if j < 8 else b[j - 8 : j - 7]
                top[j] = top[j] + a * jnp.broadcast_to(row, (8, 128))
                bot[j] = bot[j] + b * jnp.broadcast_to(row, (4, 128))
        return tuple(top), tuple(bot)

    gram_state = [
        (
            tuple(jnp.zeros((8, 128), F32) for _ in range(NB)),
            tuple(jnp.zeros((4, 128), F32) for _ in range(NB)),
        )
    ]
    steps = 1024 // GRAM_UNROLL // GRAM_PIECES
    done = [0]

    def gram():
        n = done[0]
        gram_state[0] = lax.fori_loop(n * steps, (n + 1) * steps, gram_chunk, gram_state[0])
        done[0] = n + 1

    def vblk(b):
        return vmat.at[rows(b), :]

    def mm1(bs):
        for m in range(2):
            r = slice(m * 512, (m + 1) * 512)
            p = [jnp.dot(act[r, rows(b)], vmat[rows(b), :], preferred_element_type=F32) for b in bs]
            acc[r, :] += functools.reduce(jnp.add, p)

    xp, xm, xf = mod4(x + 1), mod4(x - 1), mod4(x + 2)

    def x_right(dy):
        b = blk(x, dy, c)
        return rcopy(vblk(b), vblk(b), xr_s.at[dy], xr_r.at[dy], dev(xp, y, z, c))

    yf = dev(x, mod4(y + 2), z, c)

    def x_left(dy):
        b = blk(x, dy, c)
        return rcopy(vblk(b), vblk(b), xl_s.at[dy], xl_r.at[dy], dev(xm, y, z, c))

    def x_far(dy):
        odd = lax.rem(dy, 2)
        b = blk(mod4(x - 1 + 2 * odd), dy, c)
        return rcopy(vblk(b), vblk(b), xf_s.at[dy], xf_r.at[dy], dev(mod4(x + 1 - 2 * odd), y, z, c))

    def d2d(xo, dy):
        b = blk(mod4(x + xo), dy, c)
        return rcopy(vblk(b), vblk(b), d_s.at[xo * 4 + dy], d_r.at[xo * 4 + dy], dev(x, y, z, oc))

    def to_dy(i):
        return i + (i // 2) * (5 - 2 * i)

    ld_basis.wait()
    gram()
    gram()

    ycps = {}

    def y_send(k):
        src = vblk(b0) if k == 2 else zoth
        cp = rcopy(src, vblk(b0), ys_s.at[k], ys_r.at[4 - k], dev(x, mod4(y + k), z, c))
        cp.start()
        sends.append(cp)
        ycps[4 - k] = cp

    def own_block(dy):
        x_right(dy).start()
        x_left(dy).start()
        d2d(0, dy).start()

    def ring(dy):
        x_right(dy).wait_recv()
        x_left(dy).wait_recv()
        x_far(dy).start()
        d2d(3, dy).start()
        d2d(1, dy).start()

    def mine(*which):
        mm1([blk(xx, dy, c) for xx, dy in which])

    def others(*which):
        for xo, dy in which:
            d2d(xo, dy).wait_recv()
        mm1([blk(mod4(x + xo), dy, oc) for xo, dy in which])

    for cp in zrecvs[0]:
        cp.wait_recv()
    y_send(1)
    y_send(3)
    for cp in zrecvs[1]:
        cp.wait_recv()
    own_block(0)
    y_send(2)
    ld_act.wait()
    mine((x, 0))
    ld_rest.wait()
    gram()
    ycps[1].wait_recv()
    own_block(1)
    ycps[3].wait_recv()
    own_block(3)
    ring(0)
    gram()
    mine((x, 1), (x, 3))
    ring(1)
    mine((xm, 0), (xp, 0))
    ycps[2].wait_recv()
    own_block(2)
    mine((xm, 1), (xp, 1))
    ring(3)
    gram()
    gram()
    others((0, 0), (0, 1), (0, 3))
    gram()
    others((3, 0), (1, 0))
    mine((x, 2), (xm, 3), (xp, 3))
    ring(2)
    mine((xm, 2), (xp, 2))
    x_far(0).wait_recv()
    d2d(2, 0).start()
    mine((xf, 0))
    gram()
    x_far(1).wait_recv()
    d2d(2, 1).start()
    mine((xf, 1))
    others((3, 1), (1, 1), (0, 2), (2, 0))
    x_far(3).wait_recv()
    d2d(2, 3).start()
    mine((xf, 3))
    others((3, 3), (1, 3), (3, 2), (1, 2), (2, 1))
    x_far(2).wait_recv()
    d2d(2, 2).start()
    mine((xf, 2))
    others((2, 3), (2, 2))
    gram_state = gram_state[0]

    lane8 = lax.broadcasted_iota(jnp.int32, (8, 128), 1)
    sub8 = lax.broadcasted_iota(jnp.int32, (8, 128), 0)
    zero4 = jnp.zeros((4, 128), F32)

    def lanes(v):
        return jnp.broadcast_to(jnp.sum(v, axis=1, keepdims=True), (8, 128))

    def pad(v):
        return jnp.concatenate([v, zero4], axis=0)

    def reduce_start(stage, buf, value, ss, rs):
        me, count = ((z * 2 + c, 8), (y, 4), (x, 4))[stage]
        buf[me] = value
        cps = []
        for k in range(1, count):
            t = lax.rem(me + k, count)
            d = (
                dev(x, y, t // 2, lax.rem(t, 2)) if stage == 0 else dev(x, t, z, c) if stage == 1 else dev(t, y, z, c)
            )
            cp = rcopy(buf.at[me], buf.at[me], ss.at[k], rs.at[k], d)
            cp.start()
            cps.append(cp)
        sends.extend(cps)
        return cps, buf, count

    def reduce_end(started):
        cps, buf, count = started
        for cp in cps:
            cp.wait_recv()
        parts = [buf[k] for k in range(count)]
        while len(parts) > 1:
            parts = [parts[k] + parts[k + 1] for k in range(0, len(parts), 2)]
        return parts[0]

    gup = jnp.zeros((8, 128), F32)
    gdn = jnp.zeros((8, 128), F32)
    for j in range(NB):
        gup = jnp.where(lane8 == j, lanes(gram_state[0][j]), gup)
        gdn = jnp.where(lane8 == j, lanes(pad(gram_state[1][j])), gdn)
    gram_sum = reduce_start(0, arz, jnp.concatenate([gup, gdn], axis=0), az_s, az_r)

    ld_curv.wait()

    for m in range(4):
        r = slice(m * 256, (m + 1) * 256)
        wt[:, r] = (curv[r, :] * acc[r, :]).T.astype(BF16)

    def mm2(b):
        return jnp.dot(wt[...], act[:, rows(b)], preferred_element_type=F32)

    def d2d2(i):
        return rcopy(dsend.at[i], drecv.at[i], d2_s.at[i], d2_r.at[i], dev(x, y, z, oc))

    def idx(xo, dy):
        return xo * 4 + dy

    def other(*which):
        ps = [mm2(blk(mod4(x + xo), dy, oc)).astype(BF16) for xo, dy in which]
        for (xo, dy), p in zip(which, ps):
            dsend[idx(xo, dy)] = p
        for xo, dy in which:
            d2d2(idx(xo, dy)).start()

    def chip_sums(*which):
        ps = [mm2(blk(mod4(x + xo), dy, c)) for xo, dy in which]
        for xo, dy in which:
            d2d2(idx(xo, dy)).wait_recv()
        return [p + drecv[idx(xo, dy)].astype(F32) for (xo, dy), p in zip(which, ps)]

    def far2(dy):
        odd = lax.rem(dy, 2)
        return rcopy(xfs.at[dy], xfr.at[dy], f2_s.at[dy], f2_r.at[dy], dev(mod4(x - 1 + 2 * odd), y, z, c))

    def right2(dy):
        return rcopy(xns.at[dy], xl.at[dy], n2_s.at[dy], l2_r.at[dy], dev(xp, y, z, c))

    def left2(dy):
        return rcopy(xns.at[4 + dy], xr.at[dy], n2_s.at[4 + dy], r2_r.at[dy], dev(xm, y, z, c))

    def far_send(*dys):
        for dy, s in zip(dys, chip_sums(*((2, dy) for dy in dys))):
            if dy == 0:
                y_far(0).wait_recv()
                s = s + yfr[0].astype(F32)
            xfs[dy] = s.astype(BF16)
        for dy in dys:
            far2(dy).start()

    def near_send(*dys):
        for dy, s in zip(dys, chip_sums(*((1 + 2 * (dy % 2), dy) for dy in dys))):
            if dy == 0:
                y_far(1).wait_recv()
                s = s + yfr[1].astype(F32)
            xns[(dy % 2) * 4 + dy] = s.astype(BF16)
        for dy in dys:
            (left2 if dy % 2 else right2)(dy).start()

    def near_add(*dys):
        sums = chip_sums(*((3 - 2 * (dy % 2), dy) for dy in dys))
        for dy, s in zip(dys, sums):
            if dy != 2:
                far2(dy).wait_recv()
                s = s + xfr[dy].astype(F32)
            xns[(1 - dy % 2) * 4 + dy] = s.astype(BF16)
        for dy in dys:
            (right2 if dy % 2 else left2)(dy).start()

    def y_far(n):
        return rcopy(yfs.at[n], yfr.at[n], yf_s.at[n], yf_r.at[n], yf)

    other((2, 2), (1, 2))
    other((2, 3), (2, 1))
    other((3, 3), (3, 1))
    for n, s in enumerate(chip_sums((2, 2), (1, 2))):
        yfs[n] = s.astype(BF16)
        y_far(n).start()
    far_send(3, 1)
    near_send(3, 1)
    other((2, 0), (1, 3))
    other((3, 2), (1, 1))
    far_send(0)
    near_add(3)
    near_add(2)
    other((1, 0), (3, 0))
    near_add(1)
    other((0, 2), (0, 3))
    gram_sum = reduce_start(1, ary, reduce_end(gram_sum), ay_s, ay_r)
    near_send(0)
    other((0, 1), (0, 0))
    gram_sum = reduce_start(2, arx, reduce_end(gram_sum), ax_s, ax_r)
    x_own = dict(zip((2, 3, 1, 0), chip_sums((0, 2), (0, 3), (0, 1), (0, 0))))
    def x_sum(dy):
        left2(dy).wait_recv()
        s = x_own[dy] + xr[dy].astype(F32)
        if dy != 2:
            right2(dy).wait_recv()
            s = s + xl[dy].astype(F32)
        return s

    def y2(k):
        return rcopy(ysend.at[k], yrecv.at[4 - k], y2_s.at[k], y2_r.at[4 - k], dev(x, mod4(y + k), z, c))

    for k in (2, 3, 1):
        if k == 1:
            near_add(0)
        ysend[k] = x_sum(k).astype(BF16)
        cp = y2(k)
        cp.start()
        sends.append(cp)
    h_own = x_sum(0)
    y2(1).wait_recv()
    y2(3).wait_recv()
    h_oth = yrecv[1].astype(F32) + yrecv[3].astype(F32)
    zcps = []

    def z2(value, head, q):
        v = value.T.astype(BF16)
        for zz in range(4):
            zsend[zz, head] = v[zz * 64 : (zz + 1) * 64, :]
        for k in (2, 1, 3):
            zt = mod4(z + k)
            n = q * 3 + k - 1
            cp = rcopy(zsend.at[zt, head], zrecv.at[z, head], z2_s.at[n], z2_r.at[n], dev(x, y, zt, c))
            cp.start()
            sends.append(cp)
            zcps.append(cp)

    z2(h_oth, 1 - yl, 0)
    y2(2).wait_recv()
    z2(h_own + yrecv[2].astype(F32), yl, 1)
    zrecv[z] = zsend[z]
    for cp in zcps:
        cp.wait_recv()

    for zz in range(4):
        for hl in range(2):
            for kv in range(2):
                v = zrecv[zz, hl, :, kv * 128 : (kv + 1) * 128].astype(F32) * (1.0 / TOKENS)
                curved[pl.ds(2 * (hl * 4 + zz) + kv, 64, stride=16), :] = v

    def dot_chunk(i, carry):
        tops, bots, sq = carry
        tops, bots = list(tops), list(bots)
        for u in range(4):
            t = curved[pl.ds(pl.multiple_of(i * 32 + u * 8, 8), 8), :]
            sq = sq + t * t
            for s in range(8):
                cols = pl.ds(pl.multiple_of(i * 4096 + u * 1024 + s * 128, 128), 128)
                row = t[s : s + 1]
                tops[s % 4] = tops[s % 4] + basis[0:8, cols] * jnp.broadcast_to(row, (8, 128))
                bots[s % 4] = bots[s % 4] + basis[8:12, cols] * jnp.broadcast_to(row, (4, 128))
        return tuple(tops), tuple(bots), sq

    tops, bots, sq = lax.fori_loop(
        0,
        32,
        dot_chunk,
        (
            tuple(jnp.zeros((8, 128), F32) for _ in range(4)),
            tuple(jnp.zeros((4, 128), F32) for _ in range(4)),
            jnp.zeros((8, 128), F32),
        ),
    )
    top = (tops[0] + tops[1]) + (tops[2] + tops[3])
    bot = (bots[0] + bots[1]) + (bots[2] + bots[3])

    row = jnp.sum(
        jnp.where(lane8 == sub8, lanes(top), 0.0)
        + jnp.where(lane8 == sub8 + 8, lanes(pad(bot)), 0.0)
        + jnp.where(lane8 == NB, lanes(sq), 0.0),
        axis=0,
        keepdims=True,
    )
    row = reduce_end(reduce_start(0, crz, row, cz_s, cz_r))
    row = reduce_end(reduce_start(1, cry, row, cy_s, cy_r))
    row = reduce_end(reduce_start(2, crx, row, cx_s, cx_r))
    row = row * (1.0 / PARAMS)
    tot = reduce_end(gram_sum) * (1.0 / PARAMS)
    gt, gb = tot[0:8], tot[8:16]
    lane1 = lax.broadcasted_iota(jnp.int32, (1, 128), 1)
    crow = jnp.where(lane1 < NB, row, 0.0)
    ct = lanes(jnp.where(lane8 == sub8, jnp.broadcast_to(crow, (8, 128)), 0.0))
    cb = lanes(jnp.where(lane8 == sub8 + 8, jnp.broadcast_to(crow, (8, 128)), 0.0))
    gc = jnp.sum(gt * ct + gb * cb, axis=0, keepdims=True)
    cgc = jnp.sum(crow * gc, axis=1, keepdims=True)
    cc = jnp.sum(crow * crow, axis=1, keepdims=True)
    squares = jnp.sum(jnp.where(lane1 == NB, row, 0.0), axis=1, keepdims=True)
    norm = jnp.sqrt(squares - 2.0 * cc + cgc + 1e-06)
    inv = jnp.broadcast_to(1.0 / norm, (8, 128))
    hess_ref[...] = jnp.where(lane1 == NB, jnp.broadcast_to(norm, (1, 128)), crow)

    def res_chunk(i, _):
        for u in range(4):
            t = []
            for s in range(8):
                cols = pl.ds(pl.multiple_of(i * 4096 + u * 1024 + s * 128, 128), 128)
                t.append(basis[0:8, cols] * ct + pad(basis[8:12, cols]) * cb)
            for sh in (4, 2, 1):
                keep = lax.rem(sub8 // sh, 2) == 0
                t = [
                    jnp.where(
                        keep,
                        t[s] + pltpu.roll(t[s], 8 - sh, 0),
                        t[s + sh] + pltpu.roll(t[s + sh], sh, 0),
                    )
                    for s in range(sh)
                ]
            r = pl.ds(pl.multiple_of(i * 32 + u * 8, 8), 8)
            out_ref[r, :] = (curved[r, :] - t[0]) * inv
        return 0

    lax.fori_loop(0, 32, res_chunk, 0)

    for cp in sends:
        cp.wait_send()

    for dy in range(4):
        x_right(dy).wait_send()
        x_left(dy).wait_send()
        x_far(dy).wait_send()
        left2(dy).wait_send()
        if dy != 2:
            far2(dy).wait_send()
            right2(dy).wait_send()
        for xo in range(4):
            d2d(xo, dy).wait_send()
            d2d2(xo * 4 + dy).wait_send()
    for n in range(2):
        y_far(n).wait_send()


def body(activations, curvature, basis, krylov):
    dma = pltpu.SemaphoreType.DMA
    vm = pltpu.VMEM
    anyspace = pl.BlockSpec(memory_space=pltpu.HBM)
    vspace = pl.BlockSpec(memory_space=pltpu.VMEM)
    blocks = lambda n: vm((n, 256, 256), BF16)
    out, hess = pl.pallas_call(
        kernel,
        out_shape=(jax.ShapeDtypeStruct((1024, 128), F32), jax.ShapeDtypeStruct((1, 128), F32)),
        in_specs=[anyspace] * 4,
        out_specs=(vspace, vspace),
        scratch_shapes=[
            vm((1024, 8192), BF16),
            vm((1024, 256), F32),
            vm((NB, 131072), F32),
            vm((1024, 128), F32),
            vm((8192, 256), BF16),
            vm((4, 2, 64, 256), BF16),
            vm((256, 256), BF16),
            vm((1024, 256), F32),
            vm((256, 1024), BF16),
            blocks(16),
            blocks(16),
            blocks(4),
            blocks(8),
            blocks(4),
            blocks(4),
            blocks(4),
            blocks(4),
            blocks(4),
            vm((4, 2, 64, 256), BF16),
            vm((4, 2, 64, 256), BF16),
            vm((1024, 128), F32),
            blocks(2),
            blocks(2),
            vm((8, 16, 128), F32),
            vm((4, 16, 128), F32),
            vm((4, 16, 128), F32),
            vm((8, 1, 128), F32),
            vm((4, 1, 128), F32),
            vm((4, 1, 128), F32),
            dma((5,)),
            dma((6,)),
            dma((6,)),
            dma((4,)),
            dma((4,)),
            dma((4,)),
            dma((4,)),
            dma((4,)),
            dma((4,)),
            dma((4,)),
            dma((4,)),
            dma((16,)),
            dma((16,)),
            dma((16,)),
            dma((16,)),
            dma((4,)),
            dma((4,)),
            dma((8,)),
            dma((4,)),
            dma((4,)),
            dma((4,)),
            dma((4,)),
            dma((6,)),
            dma((6,)),
            dma((8,)),
            dma((8,)),
            dma((4,)),
            dma((4,)),
            dma((4,)),
            dma((4,)),
            dma((8,)),
            dma((8,)),
            dma((4,)),
            dma((4,)),
            dma((4,)),
            dma((4,)),
            dma((2,)),
            dma((2,)),
        ],
        compiler_params=pltpu.CompilerParams(
            collective_id=0, has_side_effects=True, vmem_limit_bytes=VMEM_BYTES
        ),
    )(activations, curvature, basis, krylov.reshape(1024, 128))
    return out.reshape(131072), hess[0, :13]


def solution(mesh):
    placed = (P("dp", None), P("dp", "mp"), P(None, ("dp", "mp")), P(("dp", "mp")))
    return jax.shard_map(
        body, mesh=mesh, in_specs=placed, out_specs=(P(("dp", "mp")), P()), check_vma=False
    )
```
